128 devices in a mesh: gx: 8 (over y, z_hi), gy: 16 (over x, z_lo, core).
Axes of the slice: x: 4, y: 4, z: 4 (z_hi: 2, z_lo: 2; z = z_hi * 2 + z_lo), core: 2. Of those that a mesh axis runs over, the one named last changes fastest.
Arguments:
- q_nodes: bfloat16 [128, 512, 4096], P(('gx', 'gy')), may hold values from -30 to 30, as said below
- k_cache: bfloat16 [128, 1024, 512], P(('gx', 'gy')), may hold values from -6 to 6, as said below
- v_cache: bfloat16 [128, 1024, 512], P(('gx', 'gy')), may hold values from -6 to 6
- k_tree: bfloat16 [128, 512, 512], P(('gx', 'gy')), may hold values from -6 to 6
- v_tree: bfloat16 [128, 512, 512], P(('gx', 'gy')), may hold values from -6 to 6
- anc_bits: int32 [128, 512, 16], P(('gx', 'gy')), may hold values from -2147483648 to 2147483647, as said below
- node_count: int32 [128], P(('gx', 'gy')), may hold values from 1 to 512, as said below
- cache_len: int32 [128], P(('gx', 'gy')), may hold values from 256 to 1024, as said below
- sinks: float32 [64], replicated, may hold values from 5 to 10
- o_weight: bfloat16 [4096, 2880], P(('gx', 'gy')), may hold values from -0.09375 to 0.09375
Outputs:
- attended: bfloat16 [128, 512, 4096], P(('gx', 'gy'))
- projected: bfloat16 [128, 512, 2880], P(('gx', 'gy'))
The draws below stay inside these ranges and needn't reach their ends.
Inputs may be any that keep to these rules, and one draw needn't show every extreme that they name: `q_nodes`: custom draw of queries. `k_cache`: custom draw of keys. `anc_bits`: bit j mod 32 of word j // 32 in row i is set exactly when tree node j is node i or one of its ancestors; node 0 is the root and a node's ancestors have lower indices. `node_count`: write request r as a * 16 + b with b < 16. Where a + b is even, the tree has more than (2) * 128 nodes; elsewhere it has at most 128. Request 0 has 512 nodes. `cache_len`: request 0 has 1024 cached positions.
All inputs are finite; a program needn't handle non-finite values.
Results may differ from the reference program's by a relative error of at most 0.0055.
Values may be sent and summed in bfloat16 or wider, within the bound.
A program may use at most 192 MiB of HBM per device.

```python
import jax
import jax.numpy as jnp
from jax import lax

QH = 64
KVH = 8
HD = 64
D = 2880
TREE_MAX = 512
BLK = 128
CACHE_MAX = 1024
REQUESTS = 128
N_GY = 16


def tree_tables(key):
    base_key = jax.random.fold_in(key, 11)
    block_count = TREE_MAX // BLK
    request_ids = jnp.arange(REQUESTS, dtype=jnp.int32)
    parity = (request_ids // N_GY + request_ids % N_GY) % 2
    busy_blocks = jax.random.randint(jax.random.fold_in(base_key, 1), (REQUESTS,), block_count - 1, block_count + 1)
    live_blocks = jnp.where(parity == 0, busy_blocks, 1).astype(jnp.int32)
    extra_nodes = jax.random.randint(jax.random.fold_in(base_key, 2), (REQUESTS,), 1, BLK + 1)
    node_total = ((live_blocks - 1) * BLK + extra_nodes).astype(jnp.int32)
    node_total = node_total.at[0].set(TREE_MAX)
    steps_back = jax.random.randint(jax.random.fold_in(base_key, 3), (REQUESTS, TREE_MAX), 1, 5)
    parents = jnp.maximum(jnp.arange(TREE_MAX, dtype=jnp.int32)[None, :] - steps_back, 0).astype(jnp.int32)
    word_count = TREE_MAX // 32
    word_ids = jnp.arange(word_count, dtype=jnp.int32)
    row_ids = jnp.arange(REQUESTS, dtype=jnp.int32)

    def add_node(node_index, bit_table):
        parent_row = bit_table[row_ids, parents[:, node_index]]
        parent_row = jnp.where(node_index > 0, parent_row, jnp.zeros_like(parent_row))
        own_bit = jnp.where(word_ids == node_index // 32, jnp.left_shift(jnp.asarray(1, jnp.int32), node_index % 32), 0).astype(jnp.int32)
        new_row = jnp.bitwise_or(parent_row, own_bit[None, :])
        return lax.dynamic_update_slice(bit_table, new_row[:, None, :], (0, node_index, 0))
    bit_table = lax.fori_loop(0, TREE_MAX, add_node, jnp.zeros((REQUESTS, TREE_MAX, word_count), jnp.int32))
    return (node_total, bit_table)


def draw_node_count(key, part):
    return tree_tables(key)[0]


def draw_anc_bits(key, part):
    return tree_tables(key)[1]


def draw_cache_len(key, part):
    counts = jax.random.randint(jax.random.fold_in(key, 41), (REQUESTS,), CACHE_MAX // 4, CACHE_MAX + 1)
    return counts.astype(jnp.int32).at[0].set(CACHE_MAX)


def draw_k_cache(key, part):
    full_shape = (REQUESTS, CACHE_MAX, KVH * HD)
    values = jnp.clip(jax.random.normal(jax.random.fold_in(key, 21), full_shape, jnp.float32), -6.0, 6.0)
    return values.astype(jnp.bfloat16)


def draw_q_nodes(key, part):
    full_shape = (REQUESTS, TREE_MAX, QH * HD)
    values = jnp.clip(2.0 * jax.random.normal(jax.random.fold_in(key, 31), full_shape, jnp.float32), -12.0, 12.0)
    return values.astype(jnp.bfloat16)


def steps_of(rng, dims, split, smallest, largest):
    gain, own = 1.0, jax.random.fold_in(rng, 6)
    for position, blocks in split:
        steps = jnp.exp(jax.random.uniform(jax.random.fold_in(own, position), (blocks,), jnp.float32, smallest / len(split), largest / len(split)))
        gain = gain * jnp.repeat(steps, dims[position] // blocks).reshape([-1 if axis == position else 1 for axis in range(len(dims))])
    return gain


def bell_draw(key, extent, spread, most, cuts=(), kind=jnp.bfloat16):
    drawn = spread * jax.random.normal(key, extent, jnp.float32)
    if cuts:
        drawn = drawn * steps_of(key, extent, cuts, -0.22, 0.18)
    return jnp.clip(drawn, -most, most).astype(kind)


def setup_inputs(seed: int = 0) -> dict:
    keys = jax.random.split(jax.random.key(seed), 11)
    q_nodes = draw_q_nodes(jax.random.fold_in(keys[10], 71), 0)
    k_cache = draw_k_cache(jax.random.fold_in(keys[10], 71), 0)
    v_cache = bell_draw(keys[2], (REQUESTS, CACHE_MAX, KVH * HD), 1.0, 6.0, ((0, 128),))
    k_tree = bell_draw(keys[3], (REQUESTS, TREE_MAX, KVH * HD), 1.0, 6.0, ((0, 128),))
    v_tree = bell_draw(keys[4], (REQUESTS, TREE_MAX, KVH * HD), 1.0, 6.0, ((0, 128),))
    anc_bits = draw_anc_bits(jax.random.fold_in(keys[10], 71), 0)
    node_count = draw_node_count(jax.random.fold_in(keys[10], 71), 0)
    cache_len = draw_cache_len(jax.random.fold_in(keys[10], 71), 0)
    sinks = jnp.clip(jax.random.uniform(keys[8], (QH,), jnp.float32, 5.0, 10.0), 5.0, 10.0)
    o_weight = bell_draw(keys[9], (QH * HD, D), (QH * HD) ** -0.5, 0.09375, ((0, 128),))
    return dict(q_nodes=q_nodes, k_cache=k_cache, v_cache=v_cache, k_tree=k_tree, v_tree=v_tree, anc_bits=anc_bits, node_count=node_count, cache_len=cache_len, sinks=sinks, o_weight=o_weight)


MASKED = -1.0e30


def unpack_bits(bit_words):
    shift_ids = jnp.arange(32, dtype=jnp.int32)
    bit_flags = jnp.bitwise_and(jnp.right_shift(bit_words[:, :, None], shift_ids), 1)
    return bit_flags.reshape(bit_words.shape[0], bit_words.shape[1] * 32) > 0


def attend_rows(q_rows, tree_ok, cache_keys, cache_values, tree_keys, tree_values, cache_count, sinks):
    row_total = q_rows.shape[0]
    groups = QH // KVH
    head_width = groups * HD
    scale_factor = HD ** -0.5
    cache_ok = jnp.arange(cache_keys.shape[0], dtype=jnp.int32) < cache_count
    tree_mask = jnp.repeat(tree_ok, groups, axis=0)

    def per_kv_head(kv_head):
        q_part = lax.dynamic_slice_in_dim(q_rows, kv_head * head_width, head_width, 1).reshape(row_total * groups, HD)
        key_cache = lax.dynamic_slice_in_dim(cache_keys, kv_head * HD, HD, 1)
        value_cache = lax.dynamic_slice_in_dim(cache_values, kv_head * HD, HD, 1)
        key_tree = lax.dynamic_slice_in_dim(tree_keys, kv_head * HD, HD, 1)
        value_tree = lax.dynamic_slice_in_dim(tree_values, kv_head * HD, HD, 1)
        score_cache = jnp.dot(q_part, key_cache.T, preferred_element_type=jnp.float32) * scale_factor
        score_cache = jnp.where(cache_ok[None, :], score_cache, MASKED)
        score_tree = jnp.dot(q_part, key_tree.T, preferred_element_type=jnp.float32) * scale_factor
        score_tree = jnp.where(tree_mask, score_tree, MASKED)
        sink_rows = jnp.tile(lax.dynamic_slice_in_dim(sinks, kv_head * groups, groups, 0), row_total)
        row_max = jnp.maximum(sink_rows, jnp.maximum(jnp.max(score_cache, axis=1), jnp.max(score_tree, axis=1)))
        weight_cache = jnp.exp(score_cache - row_max[:, None])
        weight_tree = jnp.exp(score_tree - row_max[:, None])
        denominator = jnp.exp(sink_rows - row_max) + jnp.sum(weight_cache, axis=1) + jnp.sum(weight_tree, axis=1)
        numerator = jnp.dot(weight_cache.astype(jnp.bfloat16), value_cache, preferred_element_type=jnp.float32)
        numerator = numerator + jnp.dot(weight_tree.astype(jnp.bfloat16), value_tree, preferred_element_type=jnp.float32)
        return (numerator / denominator[:, None]).reshape(row_total, head_width)

    per_head = lax.map(per_kv_head, jnp.arange(KVH, dtype=jnp.int32))
    return jnp.transpose(per_head, (1, 0, 2)).reshape(row_total, QH * HD)


def reference(q_nodes, k_cache, v_cache, k_tree, v_tree, anc_bits, node_count, cache_len, sinks, o_weight):
    def per_request(request):
        queries, cache_keys, cache_values, tree_keys, tree_values, bit_words, node_limit, cache_count = request
        result = attend_rows(queries, unpack_bits(bit_words), cache_keys, cache_values, tree_keys, tree_values, cache_count, sinks)
        node_live = jnp.arange(queries.shape[0], dtype=jnp.int32) < node_limit
        attended_rows = jnp.where(node_live[:, None], result, jnp.zeros_like(result)).astype(jnp.bfloat16)
        projected_rows = jnp.dot(attended_rows, o_weight, preferred_element_type=jnp.float32).astype(jnp.bfloat16)
        return attended_rows, projected_rows

    attended, projected = lax.map(per_request, (q_nodes, k_cache, v_cache, k_tree, v_tree, anc_bits, node_count, cache_len))
    return (attended, projected)
```

```python
import functools

import jax
import jax.numpy as jnp
from jax import lax
from jax.experimental import pallas as pl
from jax.experimental.pallas import tpu as pltpu
from jax.sharding import Mesh, PartitionSpec as P

HD = 64
NODES = 512
LIGHT = 128
CACHE = 1024
HALF = 2048
COLS = 1536
D = 2880
TILE = 256
SUMS = 16
EXP_SCALE = 0.125 * 1.4426950408889634
MASKED = -1.0e30
F32 = jnp.float32
BF16 = jnp.bfloat16


def lane_ids(shape):
    return lax.broadcasted_iota(jnp.int32, shape, len(shape) - 1)


def row_ids(shape):
    return lax.broadcasted_iota(jnp.int32, shape, len(shape) - 2)


def build_bias(bits_ref, bias_ref, keys, nodes):
    shift = row_ids((32, nodes))
    for word in range(keys // 32):
        row = jnp.broadcast_to(bits_ref[word : word + 1, :nodes], (32, nodes))
        bit = jnp.bitwise_and(lax.shift_right_logical(row, shift), 1)
        bias_ref[word * 32 : word * 32 + 32, :] = jnp.where(bit > 0, 0.0, MASKED)


def spread_keys(pair, second):
    wide = pair.astype(F32)
    turned = pltpu.roll(wide, HD, 1)
    take_own = (lane_ids(wide.shape) < HD) == jnp.logical_not(second)
    return jnp.where(take_own, wide, turned)


def turn_values(pair, second):
    turned = pair.astype(F32).T
    return jnp.where(second, turned[HD:], turned[:HD])


def prepare(k_cache, v_cache, k_tree, v_tree, length, second, keys_ref, values_ref, tree):
    keys = spread_keys(k_cache, second)
    keys_ref[pl.ds(0, CACHE), :] = jnp.where(row_ids(keys.shape) < length, keys, 0.0).astype(BF16)
    keys_ref[pl.ds(CACHE, tree), :] = spread_keys(k_tree, second).astype(BF16)
    values = turn_values(v_cache, second)
    live = lane_ids(values.shape) < length
    values_ref[pl.ds(0, HD), pl.ds(0, CACHE)] = jnp.where(live, values, 0.0).astype(BF16)
    live = lane_ids((SUMS, CACHE)) < length
    values_ref[pl.ds(HD, SUMS), pl.ds(0, CACHE)] = jnp.where(live, 1.0, 0.0).astype(BF16)
    values_ref[pl.ds(0, HD), pl.ds(CACHE, tree)] = turn_values(v_tree, second).astype(BF16)
    values_ref[pl.ds(HD, SUMS), pl.ds(CACHE, tree)] = jnp.ones((SUMS, tree), BF16)


def contract_last(a, b):
    return lax.dot_general(a, b, (((1,), (1,)), ((), ())), preferred_element_type=F32)


def attend_tile(keys_ref, values_ref, queries, bias, sink, tree, node_ok):
    cache_scores = contract_last(keys_ref[pl.ds(0, CACHE), :], queries)
    tree_scores = contract_last(keys_ref[pl.ds(CACHE, tree), :], queries) + bias
    row_max = jnp.maximum(
        jnp.max(cache_scores, axis=0, keepdims=True), jnp.max(tree_scores, axis=0, keepdims=True)
    )
    row_max = jnp.maximum(row_max, sink)
    cache_weights = jnp.exp2((cache_scores - row_max) * EXP_SCALE).astype(BF16)
    tree_weights = jnp.exp2((tree_scores - row_max) * EXP_SCALE).astype(BF16)
    sums = jnp.dot(values_ref[:, pl.ds(0, CACHE)], cache_weights, preferred_element_type=F32)
    sums += jnp.dot(values_ref[:, pl.ds(CACHE, tree)], tree_weights, preferred_element_type=F32)
    denominator = sums[HD : HD + 1] + jnp.exp2((sink - row_max) * EXP_SCALE)
    return sums[:HD] * jnp.where(node_ok, 1.0 / denominator, 0.0)


def attend_head_pair(pair, first_head, refs, counts):
    (q_busy, q_light, keys_b, values_b, keys_l, values_l, bias_b, bias_l, sinks, out_b, out_l) = refs
    count_b, count_l = counts
    lanes = pl.ds(pl.multiple_of(pair * 128, 128), 128)
    sink_even = sinks[first_head + 2 * pair] * 8.0
    sink_odd = sinks[first_head + 2 * pair + 1] * 8.0
    for tile in range(NODES // TILE):
        rows = pl.ds(tile * TILE, TILE)
        tree = (tile + 1) * TILE
        queries = q_busy[rows, lanes]
        left = lane_ids(queries.shape) < HD
        bias = bias_b[pl.ds(0, tree), rows]
        node_ok = lane_ids((1, TILE)) + tile * TILE < count_b
        zero = jnp.zeros_like(queries)
        even = attend_tile(
            keys_b, values_b, jnp.where(left, queries, zero), bias, sink_even, tree, node_ok
        )
        odd = attend_tile(
            keys_b, values_b, jnp.where(left, zero, queries), bias, sink_odd, tree, node_ok
        )
        out_b[rows, lanes] = jnp.concatenate([even, odd], axis=0).T.astype(BF16)
    queries = q_light[:, lanes]
    left = lane_ids(queries.shape) < HD
    zero = jnp.zeros_like(queries)
    both = jnp.concatenate([jnp.where(left, queries, zero), jnp.where(left, zero, queries)], axis=0)
    columns = lane_ids((1, TILE))
    sink = jnp.where(columns < LIGHT, sink_even, sink_odd)
    node_ok = jnp.where(columns < LIGHT, columns, columns - LIGHT) < count_l
    bias = jnp.concatenate([bias_l[...], bias_l[...]], axis=1)
    result = attend_tile(keys_l, values_l, both, bias, sink, LIGHT, node_ok)
    stacked = jnp.concatenate([result[:, :LIGHT], result[:, LIGHT:]], axis=0)
    out_l[:, lanes] = stacked.T.astype(BF16)


def attention_kernel(
    scalars, sinks, q_busy, q_light, kc_b, vc_b, kt_b, vt_b, kc_l, vc_l, kt_l, vt_l, bits_b, bits_l,
    out_b, out_l, keys_b, values_b, keys_l, values_l, bias_b, bias_l,
):
    build_bias(bits_b, bias_b, NODES, NODES)
    build_bias(bits_l, bias_l, LIGHT, LIGHT)
    head_base = scalars[4]
    refs = (q_busy, q_light, keys_b, values_b, keys_l, values_l, bias_b, bias_l, sinks, out_b, out_l)

    def per_kv(kv, carry):
        second = lax.rem(kv, 2) == 1
        lanes = pl.ds(pl.multiple_of(lax.div(kv, 2) * 128, 128), 128)
        prepare(
            kc_b[:, lanes], vc_b[:, lanes], kt_b[:, lanes], vt_b[:, lanes], scalars[1], second,
            keys_b, values_b, NODES,
        )
        prepare(
            kc_l[:, lanes], vc_l[:, lanes], kt_l[:, lanes], vt_l[:, lanes], scalars[3], second,
            keys_l, values_l, LIGHT,
        )

        def per_pair(step, inner):
            attend_head_pair(kv * 4 + step, head_base, refs, (scalars[0], scalars[2]))
            return inner

        return lax.fori_loop(0, 4, per_pair, carry)

    lax.fori_loop(0, 4, per_kv, 0)


def attention(scalars, sinks, *arrays):
    vmem = pl.BlockSpec(memory_space=pltpu.VMEM)
    smem = pl.BlockSpec(memory_space=pltpu.SMEM)
    return pl.pallas_call(
        attention_kernel,
        out_shape=(
            jax.ShapeDtypeStruct((NODES, HALF), BF16),
            jax.ShapeDtypeStruct((LIGHT, HALF), BF16),
        ),
        in_specs=[smem, smem] + [vmem] * len(arrays),
        out_specs=(vmem, vmem),
        scratch_shapes=[
            pltpu.VMEM((CACHE + NODES, 128), BF16),
            pltpu.VMEM((HD + SUMS, CACHE + NODES), BF16),
            pltpu.VMEM((CACHE + LIGHT, 128), BF16),
            pltpu.VMEM((HD + SUMS, CACHE + LIGHT), BF16),
            pltpu.VMEM((NODES, NODES), F32),
            pltpu.VMEM((LIGHT, LIGHT), F32),
        ],
        compiler_params=pltpu.CompilerParams(vmem_limit_bytes=60 * 1024 * 1024),
        cost_estimate=pl.CostEstimate(
            flops=32 * (512 * 1536 + 128 * 1152) * 256, bytes_accessed=8 * 2**20, transcendentals=0
        ),
        name="attend",
    )(scalars, sinks, *arrays)


def on_device(
    q_nodes, k_cache, v_cache, k_tree, v_tree, anc_bits, node_count, cache_len, sinks, o_weight
):
    core = lax.axis_index("core")
    swap = lambda x: lax.ppermute(x, "core", [(0, 1), (1, 0)])
    busy = lax.rem(lax.axis_index("gx") + core, 2) == 0

    def halves(x, width):
        first, second = x[..., :width], x[..., width:]
        return jnp.where(core == 0, first, second), jnp.where(core == 0, second, first)

    weight = jnp.pad(o_weight, ((0, 0), (0, 2 * COLS - D)))
    own_columns, other_columns = halves(weight, COLS)
    got_columns = swap(other_columns)
    chip_rows = jnp.where(
        core == 0,
        jnp.concatenate([own_columns, got_columns], axis=0),
        jnp.concatenate([got_columns, own_columns], axis=0),
    )
    gathered = lax.all_gather(chip_rows, ("gx", "gyc"), axis=0, tiled=True)

    own, sent = [], []
    for x, width in (
        (q_nodes[0], HALF), (k_cache[0], 256), (v_cache[0], 256), (k_tree[0], 256), (v_tree[0], 256)
    ):
        mine, other = halves(x, width)
        own.append(mine)
        sent.append(other)
    bits = anc_bits[0].T
    counts = jnp.stack([node_count[0], cache_len[0]])
    got = swap(tuple(sent) + (bits, counts))
    own = tuple(own) + (bits, counts)
    pick_b = [jnp.where(busy, a, b) for a, b in zip(own, got)]
    pick_l = [jnp.where(busy, b, a) for a, b in zip(own, got)]
    q_b, kc_b, vc_b, kt_b, vt_b, bits_b, counts_b = pick_b
    q_l, kc_l, vc_l, kt_l, vt_l, bits_l, counts_l = pick_l
    scalars = jnp.concatenate([counts_b, counts_l, (core * 32)[None].astype(jnp.int32)])
    att_b, att_l = attention(
        scalars, sinks, q_b, q_l[:LIGHT], kc_b, vc_b, kt_b, vt_b, kc_l, vc_l, kt_l[:LIGHT],
        vt_l[:LIGHT], bits_b, bits_l,
    )
    halves_own = jnp.concatenate([att_b, att_l], axis=0)
    halves_got = swap(halves_own)
    rows = jnp.where(
        core == 0,
        jnp.concatenate([halves_own, halves_got], axis=1),
        jnp.concatenate([halves_got, halves_own], axis=1),
    )
    out = jnp.dot(rows, gathered, preferred_element_type=F32).astype(BF16)
    out_got = swap(out)
    out = jnp.where(
        core == 0,
        jnp.concatenate([out, out_got], axis=1),
        jnp.concatenate([out_got, out], axis=1),
    )[:, :D]

    def place(x):
        light = jnp.pad(x[NODES:], ((0, NODES - LIGHT), (0, 0)))
        return jnp.where(busy, x[:NODES], light)[None]

    return place(rows), place(out)


def solution(mesh):
    split = Mesh(mesh.devices.reshape(8, 8, 2), ("gx", "gyc", "core"))
    every = ("gx", "gyc", "core")
    placed = tuple([P(every)] * 8) + (P(), P(every))
    return jax.shard_map(
        on_device, mesh=split, in_specs=placed, out_specs=(P(every), P(every)), check_vma=False
    )
```

```python
import functools

import jax
import jax.numpy as jnp
from jax import lax
from jax.experimental import pallas as pl
from jax.experimental.pallas import tpu as pltpu
from jax.sharding import Mesh, PartitionSpec as P

HD = 64
NODES = 512
LIGHT = 128
CACHE = 1024
HALF = 2048
COLS = 1536
D = 2880
TILE = 256
SUMS = 16
EXP_SCALE = 0.125 * 1.4426950408889634
MASKED = -1.0e30
PART = 512
ROUND_AT = (1, 2, 4, 6, 11)
F32 = jnp.float32
BF16 = jnp.bfloat16


def lane_ids(shape):
    return lax.broadcasted_iota(jnp.int32, shape, len(shape) - 1)


def row_ids(shape):
    return lax.broadcasted_iota(jnp.int32, shape, len(shape) - 2)


def build_bias(bits_ref, bias_ref, keys, nodes):
    shift = row_ids((32, nodes))
    for word in range(keys // 32):
        row = jnp.broadcast_to(bits_ref[word : word + 1, :nodes], (32, nodes))
        bit = jnp.bitwise_and(lax.shift_right_logical(row, shift), 1)
        bias_ref[word * 32 : word * 32 + 32, :] = jnp.where(bit > 0, 0.0, MASKED)


def spread_keys(pair, second):
    wide = pair.astype(F32)
    turned = pltpu.roll(wide, HD, 1)
    take_own = (lane_ids(wide.shape) < HD) == jnp.logical_not(second)
    return jnp.where(take_own, wide, turned)


def turn_values(pair, second):
    turned = pair.astype(F32).T
    return jnp.where(second, turned[HD:], turned[:HD])


def prepare(k_cache, v_cache, k_tree, v_tree, length, second, keys_ref, values_ref, tree):
    keys = spread_keys(k_cache, second)
    keys_ref[pl.ds(0, CACHE), :] = jnp.where(row_ids(keys.shape) < length, keys, 0.0).astype(BF16)
    keys_ref[pl.ds(CACHE, tree), :] = spread_keys(k_tree, second).astype(BF16)
    values = turn_values(v_cache, second)
    live = lane_ids(values.shape) < length
    values_ref[pl.ds(0, HD), pl.ds(0, CACHE)] = jnp.where(live, values, 0.0).astype(BF16)
    live = lane_ids((SUMS, CACHE)) < length
    values_ref[pl.ds(HD, SUMS), pl.ds(0, CACHE)] = jnp.where(live, 1.0, 0.0).astype(BF16)
    values_ref[pl.ds(0, HD), pl.ds(CACHE, tree)] = turn_values(v_tree, second).astype(BF16)
    values_ref[pl.ds(HD, SUMS), pl.ds(CACHE, tree)] = jnp.ones((SUMS, tree), BF16)


def contract_last(a, b):
    return lax.dot_general(a, b, (((1,), (1,)), ((), ())), preferred_element_type=F32)


def attend_tile(keys_ref, values_ref, queries, bias, sink, tree, node_ok):
    cache_scores = contract_last(keys_ref[pl.ds(0, CACHE), :], queries)
    tree_scores = contract_last(keys_ref[pl.ds(CACHE, tree), :], queries) + bias
    row_max = jnp.maximum(
        jnp.max(cache_scores, axis=0, keepdims=True), jnp.max(tree_scores, axis=0, keepdims=True)
    )
    row_max = jnp.maximum(row_max, sink)
    cache_weights = jnp.exp2((cache_scores - row_max) * EXP_SCALE).astype(BF16)
    tree_weights = jnp.exp2((tree_scores - row_max) * EXP_SCALE).astype(BF16)
    sums = jnp.dot(values_ref[:, pl.ds(0, CACHE)], cache_weights, preferred_element_type=F32)
    sums += jnp.dot(values_ref[:, pl.ds(CACHE, tree)], tree_weights, preferred_element_type=F32)
    denominator = sums[HD : HD + 1] + jnp.exp2((sink - row_max) * EXP_SCALE)
    return sums[:HD] * jnp.where(node_ok, 1.0 / denominator, 0.0)


def attend_head_pair(pair, first_head, refs, counts):
    (q_busy, q_light, keys_b, values_b, keys_l, values_l, bias_b, bias_l, sinks, out_b, out_l) = refs
    count_b, count_l = counts
    lanes = pl.ds(pl.multiple_of(pair * 128, 128), 128)
    sink_even = sinks[first_head + 2 * pair] * 8.0
    sink_odd = sinks[first_head + 2 * pair + 1] * 8.0
    for tile in range(NODES // TILE):
        rows = pl.ds(tile * TILE, TILE)
        tree = (tile + 1) * TILE
        queries = q_busy[rows, lanes]
        left = lane_ids(queries.shape) < HD
        bias = bias_b[pl.ds(0, tree), rows]
        node_ok = lane_ids((1, TILE)) + tile * TILE < count_b
        zero = jnp.zeros_like(queries)
        even = attend_tile(
            keys_b, values_b, jnp.where(left, queries, zero), bias, sink_even, tree, node_ok
        )
        odd = attend_tile(
            keys_b, values_b, jnp.where(left, zero, queries), bias, sink_odd, tree, node_ok
        )
        out_b[rows, lanes] = jnp.concatenate([even, odd], axis=0).T.astype(BF16)
    queries = q_light[:, lanes]
    left = lane_ids(queries.shape) < HD
    zero = jnp.zeros_like(queries)
    both = jnp.concatenate([jnp.where(left, queries, zero), jnp.where(left, zero, queries)], axis=0)
    columns = lane_ids((1, TILE))
    sink = jnp.where(columns < LIGHT, sink_even, sink_odd)
    node_ok = jnp.where(columns < LIGHT, columns, columns - LIGHT) < count_l
    bias = jnp.concatenate([bias_l[...], bias_l[...]], axis=1)
    result = attend_tile(keys_l, values_l, both, bias, sink, LIGHT, node_ok)
    stacked = jnp.concatenate([result[:, :LIGHT], result[:, LIGHT:]], axis=0)
    out_l[:, lanes] = stacked.T.astype(BF16)


class Ring:
    def __init__(self, order, place, core):
        self.order, self.place, self.core = order, place, core

    def device(self, dim, by):
        at = dict(self.place)
        at[dim] = lax.rem(at[dim] + 4 + by, 4)
        x, y, z = at["x"], at["y"], at["z"]
        return (y * 2 + lax.div(z, 2), x * 2 + lax.rem(z, 2), self.core)

    def slab(self, ref, phase, by, half):
        dim = self.order[phase]
        at = dict(self.place)
        at[dim] = lax.rem(at[dim] + 4 + by, 4)
        index = [at["y"], lax.div(at["z"], 2), at["x"], lax.rem(at["z"], 2), slice(None)]
        full = self.order[:phase]
        where = {"x": (2,), "y": (0,), "z": (1, 3)}
        for name in full:
            for axis in where[name]:
                index[axis] = slice(None)
        if half is not None:
            axis = where[full[0]][0] if full else 4
            size = {0: 4, 1: 2, 2: 4, 4: 64}[axis] // 2
            index[axis] = pl.ds(half * size, size)
        return ref.at[tuple(index)]


def ring_copies(rings, chunks, gathered, send_sems, recv_sems, number):
    phase, step = divmod(number, 2)
    copies = []
    for part, ring in enumerate(rings):
        for side, by in enumerate((1, -1)):
            if step == 0:
                target = ring.slab(gathered[part], phase, 0, None)
                source = chunks.at[part] if phase == 0 else target
            else:
                target = ring.slab(gathered[part], phase, -by, side)
                source = target
            copies.append(
                pltpu.make_async_remote_copy(
                    src_ref=source,
                    dst_ref=target,
                    send_sem=send_sems.at[number, part, side],
                    recv_sem=recv_sems.at[number, part, side],
                    device_id=ring.device(ring.order[phase], by),
                    device_id_type=pl.DeviceIdType.MESH,
                )
            )
    return copies


def attention_kernel(
    scalars, sinks, chunks, q_busy, q_light, kc_b, vc_b, kt_b, vt_b, kc_l, vc_l, kt_l, vt_l,
    bits_b, bits_l, out_b, out_l, gather_0, gather_1, gather_2, keys_b, values_b, keys_l, values_l,
    bias_b, bias_l, send_sems, recv_sems, own_sems,
):
    gx, gyc, core = lax.axis_index("gx"), lax.axis_index("gyc"), lax.axis_index("core")
    place = {
        "x": lax.div(gyc, 2), "y": lax.div(gx, 2), "z": lax.rem(gx, 2) * 2 + lax.rem(gyc, 2)
    }
    rings = [Ring(order, place, core) for order in ("xyz", "yzx", "zxy")]
    gathered = (gather_0, gather_1, gather_2)

    barrier = pltpu.get_barrier_semaphore()
    for dim in "xyz":
        for by in (1, -1):
            pl.semaphore_signal(
                barrier, inc=1, device_id=rings[0].device(dim, by),
                device_id_type=pl.DeviceIdType.MESH,
            )
    pl.semaphore_wait(barrier, 6)

    def ring_round(number):
        return ring_copies(rings, chunks, gathered, send_sems, recv_sems, number)

    own = [
        pltpu.make_async_copy(
            chunks.at[part], rings[part].slab(gathered[part], 0, 0, None), own_sems.at[part]
        )
        for part in range(3)
    ]
    for copy in ring_round(0) + own:
        copy.start()

    build_bias(bits_b, bias_b, NODES, NODES)
    build_bias(bits_l, bias_l, LIGHT, LIGHT)
    head_base = core * 32
    refs = (q_busy, q_light, keys_b, values_b, keys_l, values_l, bias_b, bias_l, sinks, out_b, out_l)

    def per_pair(step, carry):
        kv = lax.div(step, 4)

        for number, when in enumerate(ROUND_AT):
            @pl.when(step == when)
            def _():
                for copy in ring_round(number):
                    copy.wait()
                if number == 0:
                    for copy in own:
                        copy.wait()
                for copy in ring_round(number + 1):
                    copy.start()

        @pl.when(lax.rem(step, 4) == 0)
        def _():
            second = lax.rem(kv, 2) == 1
            lanes = pl.ds(pl.multiple_of(lax.div(kv, 2) * 128, 128), 128)
            prepare(
                kc_b[:, lanes], vc_b[:, lanes], kt_b[:, lanes], vt_b[:, lanes], scalars[1], second,
                keys_b, values_b, NODES,
            )
            prepare(
                kc_l[:, lanes], vc_l[:, lanes], kt_l[:, lanes], vt_l[:, lanes], scalars[3], second,
                keys_l, values_l, LIGHT,
            )

        attend_head_pair(step, head_base, refs, (scalars[0], scalars[2]))
        return carry

    lax.fori_loop(0, 16, per_pair, 0)
    for copy in ring_round(5):
        copy.wait()


def attention(scalars, sinks, chunks, *arrays):
    vmem = pl.BlockSpec(memory_space=pltpu.VMEM)
    smem = pl.BlockSpec(memory_space=pltpu.SMEM)
    hbm = pl.BlockSpec(memory_space=pl.ANY)
    return pl.pallas_call(
        attention_kernel,
        out_shape=(
            jax.ShapeDtypeStruct((NODES, HALF), BF16),
            jax.ShapeDtypeStruct((LIGHT, HALF), BF16),
        )
        + (jax.ShapeDtypeStruct((4, 2, 4, 2, 64, PART), BF16),) * 3,
        in_specs=[smem, smem] + [vmem] * (len(arrays) + 1),
        out_specs=(vmem, vmem, hbm, hbm, hbm),
        scratch_shapes=[
            pltpu.VMEM((CACHE + NODES, 128), BF16),
            pltpu.VMEM((HD + SUMS, CACHE + NODES), BF16),
            pltpu.VMEM((CACHE + LIGHT, 128), BF16),
            pltpu.VMEM((HD + SUMS, CACHE + LIGHT), BF16),
            pltpu.VMEM((NODES, NODES), F32),
            pltpu.VMEM((LIGHT, LIGHT), F32),
            pltpu.SemaphoreType.DMA((6, 3, 2)),
            pltpu.SemaphoreType.DMA((6, 3, 2)),
            pltpu.SemaphoreType.DMA((3,)),
        ],
        compiler_params=pltpu.CompilerParams(
            vmem_limit_bytes=60 * 1024 * 1024, collective_id=0, has_side_effects=True
        ),
        cost_estimate=pl.CostEstimate(
            flops=32 * (512 * 1536 + 128 * 1152) * 256, bytes_accessed=8 * 2**20, transcendentals=0
        ),
        name="attend",
    )(scalars, sinks, chunks, *arrays)


def on_device(
    q_nodes, k_cache, v_cache, k_tree, v_tree, anc_bits, node_count, cache_len, sinks, o_weight
):
    core = lax.axis_index("core")
    swap = lambda x: lax.ppermute(x, "core", [(0, 1), (1, 0)])
    busy = lax.rem(lax.axis_index("gx") + core, 2) == 0

    def halves(x, width):
        first, second = x[..., :width], x[..., width:]
        return jnp.where(core == 0, first, second), jnp.where(core == 0, second, first)

    weight = jnp.pad(o_weight, ((0, 0), (0, 2 * COLS - D)))
    own_columns, other_columns = halves(weight, COLS)
    got_columns = swap(other_columns)
    chip_rows = jnp.where(
        core == 0,
        jnp.concatenate([own_columns, got_columns], axis=0),
        jnp.concatenate([got_columns, own_columns], axis=0),
    )
    chunks = jnp.transpose(chip_rows.reshape(64, 3, PART), (1, 0, 2))

    own, sent = [], []
    for x, width in (
        (q_nodes[0], HALF), (k_cache[0], 256), (v_cache[0], 256), (k_tree[0], 256), (v_tree[0], 256)
    ):
        mine, other = halves(x, width)
        own.append(mine)
        sent.append(other)
    bits = anc_bits[0].T
    counts = jnp.stack([node_count[0], cache_len[0]])
    got = swap(tuple(sent) + (bits, counts))
    own = tuple(own) + (bits, counts)
    pick_b = [jnp.where(busy, a, b) for a, b in zip(own, got)]
    pick_l = [jnp.where(busy, b, a) for a, b in zip(own, got)]
    q_b, kc_b, vc_b, kt_b, vt_b, bits_b, counts_b = pick_b
    q_l, kc_l, vc_l, kt_l, vt_l, bits_l, counts_l = pick_l
    scalars = jnp.concatenate([counts_b, counts_l])
    att_b, att_l, *gathered = attention(
        scalars, sinks, chunks, q_b, q_l[:LIGHT], kc_b, vc_b, kt_b, vt_b, kc_l, vc_l, kt_l[:LIGHT],
        vt_l[:LIGHT], bits_b, bits_l,
    )
    halves_own = jnp.concatenate([att_b, att_l], axis=0)
    halves_got = swap(halves_own)
    rows = jnp.where(
        core == 0,
        jnp.concatenate([halves_own, halves_got], axis=1),
        jnp.concatenate([halves_got, halves_own], axis=1),
    )
    out = jnp.concatenate(
        [
            jnp.dot(rows, part.reshape(4096, PART), preferred_element_type=F32).astype(BF16)
            for part in gathered
        ],
        axis=1,
    )
    out_got = swap(out)
    out = jnp.where(
        core == 0,
        jnp.concatenate([out, out_got], axis=1),
        jnp.concatenate([out_got, out], axis=1),
    )[:, :D]

    def place(x):
        light = jnp.pad(x[NODES:], ((0, NODES - LIGHT), (0, 0)))
        return jnp.where(busy, x[:NODES], light)[None]

    return place(rows), place(out)


def solution(mesh):
    split = Mesh(mesh.devices.reshape(8, 8, 2), ("gx", "gyc", "core"))
    every = ("gx", "gyc", "core")
    placed = tuple([P(every)] * 8) + (P(), P(every))
    return jax.shard_map(
        on_device, mesh=split, in_specs=placed, out_specs=(P(every), P(every)), check_vma=False
    )
```

```python
import functools

import jax
import jax.numpy as jnp
from jax import lax
from jax.experimental import pallas as pl
from jax.experimental.pallas import tpu as pltpu
from jax.sharding import Mesh, PartitionSpec as P

HD = 64
NODES = 512
LIGHT = 128
CACHE = 1024
HALF = 2048
COLS = 1536
D = 2880
TILE = 256
SUMS = 16
EXP_SCALE = 0.125 * 1.4426950408889634
MASKED = -1.0e30
PART = 512
MESH = pl.DeviceIdType.MESH
WHERE = {"x": (2,), "y": (0,), "z": (1, 3)}
SIZES = (4, 2, 4, 2)
PLAN = (
    (1, ("own",), ("far",)),
    (2, ("far",), ("line", "face0")),
    (4, ("line",), ("line2", "face-", "face+")),
    (5, ("face0",), ("back0",)),
    (6, ("line2",), ("face2",)),
    (9, ("face-", "face+"), ("back-", "back+")),
    (11, ("face2",), ("back2",)),
)
NAMES = (
    "own", "far", "line", "line2", "face0", "face-", "face+", "face2", "back0", "back-", "back+",
    "back2",
)
LINES = {"0": 0, "-": -1, "+": 1, "2": 2}
F32 = jnp.float32
BF16 = jnp.bfloat16


def lane_ids(shape):
    return lax.broadcasted_iota(jnp.int32, shape, len(shape) - 1)


def row_ids(shape):
    return lax.broadcasted_iota(jnp.int32, shape, len(shape) - 2)


def build_bias(bits_ref, bias_ref, keys, nodes):
    shift = row_ids((32, nodes))
    for word in range(keys // 32):
        row = jnp.broadcast_to(bits_ref[word : word + 1, :nodes], (32, nodes))
        bit = jnp.bitwise_and(lax.shift_right_logical(row, shift), 1)
        bias_ref[word * 32 : word * 32 + 32, :] = jnp.where(bit > 0, 0.0, MASKED)


def spread_keys(pair, second):
    wide = pair.astype(F32)
    turned = pltpu.roll(wide, HD, 1)
    take_own = (lane_ids(wide.shape) < HD) == jnp.logical_not(second)
    return jnp.where(take_own, wide, turned)


def turn_values(pair, second):
    turned = pair.astype(F32).T
    return jnp.where(second, turned[HD:], turned[:HD])


def prepare(k_cache, v_cache, k_tree, v_tree, length, second, keys_ref, values_ref, tree):
    keys = spread_keys(k_cache, second)
    keys_ref[pl.ds(0, CACHE), :] = jnp.where(row_ids(keys.shape) < length[:, :128], keys, 0.0).astype(BF16)
    keys_ref[pl.ds(CACHE, tree), :] = spread_keys(k_tree, second).astype(BF16)
    values = turn_values(v_cache, second)
    live = lane_ids(values.shape) < length
    values_ref[pl.ds(0, HD), pl.ds(0, CACHE)] = jnp.where(live, values, 0.0).astype(BF16)
    live = lane_ids((SUMS, CACHE)) < length
    values_ref[pl.ds(HD, SUMS), pl.ds(0, CACHE)] = jnp.where(live, 1.0, 0.0).astype(BF16)
    values_ref[pl.ds(0, HD), pl.ds(CACHE, tree)] = turn_values(v_tree, second).astype(BF16)
    values_ref[pl.ds(HD, SUMS), pl.ds(CACHE, tree)] = jnp.ones((SUMS, tree), BF16)


def contract_last(a, b):
    return lax.dot_general(a, b, (((1,), (1,)), ((), ())), preferred_element_type=F32)


def attend_tile(keys_ref, values_ref, queries, bias, sink, tree, node_ok):
    cache_scores = contract_last(keys_ref[pl.ds(0, CACHE), :], queries)
    tree_scores = contract_last(keys_ref[pl.ds(CACHE, tree), :], queries) + bias
    row_max = jnp.maximum(
        jnp.max(cache_scores, axis=0, keepdims=True), jnp.max(tree_scores, axis=0, keepdims=True)
    )
    row_max = jnp.maximum(row_max, sink)
    cache_weights = jnp.exp2((cache_scores - row_max) * EXP_SCALE).astype(BF16)
    tree_weights = jnp.exp2((tree_scores - row_max) * EXP_SCALE).astype(BF16)
    sums = jnp.dot(values_ref[:, pl.ds(0, CACHE)], cache_weights, preferred_element_type=F32)
    sums += jnp.dot(values_ref[:, pl.ds(CACHE, tree)], tree_weights, preferred_element_type=F32)
    denominator = sums[HD : HD + 1] + jnp.exp2((sink - row_max) * EXP_SCALE)
    return sums[:HD] * jnp.where(node_ok, 1.0 / denominator, 0.0)


def attend_head_pair(pair, core, refs, counts):
    (q_busy, q_light, keys_b, values_b, keys_l, values_l, bias_b, bias_l, sinks, att) = refs
    count_b, count_l = counts
    lanes = pl.ds(pl.multiple_of(pair * 128, 128), 128)
    out_lanes = pl.ds(pl.multiple_of(core * HALF + pair * 128, 128), 128)
    first_head = core * 32
    sink_even = sinks[first_head + 2 * pair] * 8.0
    sink_odd = sinks[first_head + 2 * pair + 1] * 8.0
    for tile in range(NODES // TILE):
        rows = pl.ds(tile * TILE, TILE)
        tree = (tile + 1) * TILE
        queries = q_busy[rows, lanes]
        left = lane_ids(queries.shape) < HD
        bias = bias_b[pl.ds(0, tree), rows]
        node_ok = lane_ids((1, TILE)) + tile * TILE < count_b
        zero = jnp.zeros_like(queries)
        even = attend_tile(
            keys_b, values_b, jnp.where(left, queries, zero), bias, sink_even, tree, node_ok
        )
        odd = attend_tile(
            keys_b, values_b, jnp.where(left, zero, queries), bias, sink_odd, tree, node_ok
        )
        att[rows, out_lanes] = jnp.concatenate([even, odd], axis=0).T.astype(BF16)
    queries = q_light[:, lanes]
    left = lane_ids(queries.shape) < HD
    zero = jnp.zeros_like(queries)
    both = jnp.concatenate([jnp.where(left, queries, zero), jnp.where(left, zero, queries)], axis=0)
    columns = lane_ids((1, TILE))
    sink = jnp.where(columns < LIGHT, sink_even, sink_odd)
    node_ok = jnp.where(columns < LIGHT, columns, columns - LIGHT) < count_l
    bias = jnp.concatenate([bias_l[...], bias_l[...]], axis=1)
    result = attend_tile(keys_l, values_l, both, bias, sink, LIGHT, node_ok)
    stacked = jnp.concatenate([result[:, :LIGHT], result[:, LIGHT:]], axis=0)
    att[pl.ds(NODES, LIGHT), out_lanes] = stacked.T.astype(BF16)


class Ring:
    def __init__(self, order, place, core, weights):
        self.order, self.place, self.core, self.weights = order, place, core, weights

    def moved(self, dim, by):
        return lax.rem(self.place[dim] + 4 + by, 4)

    def device(self, dim, by):
        at = dict(self.place)
        at[dim] = self.moved(dim, by)
        x, y, z = at["x"], at["y"], at["z"]
        return (y * 2 + lax.div(z, 2), x * 2 + lax.rem(z, 2), self.core)

    def block(self, offsets, whole=False, half=None):
        at = {dim: self.moved(dim, by) for dim, by in zip(self.order, offsets)}
        index = [at["y"], lax.div(at["z"], 2), at["x"], lax.rem(at["z"], 2), slice(None)]
        axes = WHERE[self.order[0]] if whole else (4,)
        if whole:
            for axis in axes:
                index[axis] = slice(None)
        if half is not None:
            size = (SIZES[axes[0]] if whole else 64) // 2
            index[axes[0]] = pl.ds(half * size, size)
        return self.weights.at[tuple(index)]

    def send(self, name, side):
        by = (1, -1)[side]
        if name == "own":
            return 0, self.block((0, 0, 0))
        if name == "far":
            return 0, self.block((-by, 0, 0), half=side)
        if name == "line":
            return 1, self.block((0, 0, 0), whole=True)
        if name == "line2":
            return 1, self.block((0, -by, 0), whole=True, half=side)
        line = LINES[name[-1]]
        if name.startswith("face"):
            return 2, self.block((0, line, 0), whole=True)
        return 2, self.block((0, line, -by), whole=True, half=side)


def message(rings, name, send_sems, recv_sems):
    number = NAMES.index(name)
    copies = []
    for part, ring in enumerate(rings):
        for side in range(2):
            axis, block = ring.send(name, side)
            copies.append(
                pltpu.make_async_remote_copy(
                    src_ref=block, dst_ref=block,
                    send_sem=send_sems.at[number, part, side],
                    recv_sem=recv_sems.at[number, part, side],
                    device_id=ring.device(ring.order[axis], (1, -1)[side]),
                    device_id_type=MESH,
                )
            )
    return copies


def whole_kernel(
    sinks, q_hbm, kc_hbm, vc_hbm, kt_hbm, vt_hbm, meta_hbm, w_hbm, att_hbm, proj_hbm,
    q_b, kc_b, vc_b, kt_b, vt_b, meta_b, q_l, kc_l, vc_l, kt_l, vt_l, meta_l,
    weights_0, weights_1, weights_2, att, proj, keys_b, values_b, keys_l, values_l, bias_b, bias_l,
    send_sems, recv_sems, load_sems, load_send, load_recv, w_sems, att_send, att_recv, att_sem,
    proj_send, proj_recv, proj_sem,
):
    gx, gyc, core = lax.axis_index("gx"), lax.axis_index("gyc"), lax.axis_index("core")
    partner = (gx, gyc, 1 - core)
    busy = lax.rem(gx + core, 2) == 0
    place = {
        "x": lax.div(gyc, 2), "y": lax.div(gx, 2), "z": lax.rem(gx, 2) * 2 + lax.rem(gyc, 2)
    }
    weights = (weights_0, weights_1, weights_2)
    rings = [Ring(order, place, core, w) for order, w in zip(("xyz", "yzx", "zxy"), weights)]

    def by_role(run):
        pl.when(busy)(lambda: run(True))
        pl.when(jnp.logical_not(busy))(lambda: run(False))

    def to_partner(source, target, send, recv):
        return pltpu.make_async_remote_copy(
            src_ref=source, dst_ref=target, send_sem=send, recv_sem=recv, device_id=partner,
            device_id_type=MESH,
        )

    def load_pairs(heavy, piece, half):
        rows, q, kc, vc, kt, vt, meta = (
            (NODES, q_b, kc_b, vc_b, kt_b, vt_b, meta_b)
            if heavy
            else (LIGHT, q_l, kc_l, vc_l, kt_l, vt_l, meta_l)
        )
        if piece[0] == "q":
            return [
                (
                    q_hbm.at[pl.ds(0, rows), pl.ds(half * HALF + piece[1] * 512, 512)],
                    q.at[:, pl.ds(pl.multiple_of(piece[1] * 512, 512), 512)],
                )
            ]
        if piece[0] == "meta":
            return [(meta_hbm, meta)]
        source = pl.ds(half * 256 + piece[1] * 128, 128)
        target = pl.ds(pl.multiple_of(piece[1] * 128, 128), 128)
        return [
            (kc_hbm.at[:, source], kc.at[:, target]),
            (vc_hbm.at[:, source], vc.at[:, target]),
            (kt_hbm.at[pl.ds(0, rows), source], kt.at[:, target]),
            (vt_hbm.at[pl.ds(0, rows), source], vt.at[:, target]),
        ]

    def slot(piece):
        return {"meta": 0, "q": 1, "kv": 5}[piece[0]] + piece[1] * (4 if piece[0] == "kv" else 1)

    def local_loads(heavy, piece):
        pairs = load_pairs(heavy, piece, core)
        return [
            pltpu.make_async_copy(a, b, load_sems.at[slot(piece) + i])
            for i, (a, b) in enumerate(pairs)
        ]

    def remote_loads(heavy, piece):
        pairs = load_pairs(heavy, piece, 1 - core)
        return [
            to_partner(a, b, load_send.at[slot(piece) + i], load_recv.at[slot(piece) + i])
            for i, (a, b) in enumerate(pairs)
        ]

    def start_loads(heavy):
        pieces = [("meta", 0), ("kv", 0)] + [("q", kv) for kv in range(4)]
        pieces.insert(5, ("kv", 1))
        for piece in pieces:
            for copy in remote_loads(heavy, piece) + local_loads(heavy, piece):
                copy.start()

    def wait_loads(piece):
        def run(heavy):
            for copy in local_loads(heavy, piece):
                copy.wait()
            for copy in remote_loads(not heavy, piece):
                copy.wait_recv()

        by_role(run)

    def wait_sends():
        def run(heavy):
            for piece in [("meta", 0)] + [("q", kv) for kv in range(4)] + [("kv", 0), ("kv", 1)]:
                for copy in remote_loads(heavy, piece):
                    copy.wait_send()

        by_role(run)

    barrier = pltpu.get_barrier_semaphore()
    for dim in "xyz":
        for by in (1, -1):
            pl.semaphore_signal(
                barrier, inc=1, device_id=rings[0].device(dim, by), device_id_type=MESH
            )
    pl.semaphore_signal(barrier, inc=1, device_id=partner, device_id_type=MESH)
    pl.semaphore_wait(barrier, 7)

    rows = pl.ds(pl.multiple_of(core * 32, 32), 32)
    chunk_local, chunk_remote = [], []
    for part, ring in enumerate(rings):
        target = ring.block((0, 0, 0)).at[rows]
        chunk_local.append(
            pltpu.make_async_copy(w_hbm.at[core, part], target, w_sems.at[0, part])
        )
        chunk_remote.append(
            to_partner(w_hbm.at[1 - core, part], target, w_sems.at[1, part], w_sems.at[2, part])
        )
    for copy in chunk_remote + chunk_local:
        copy.start()
    by_role(start_loads)
    for local, remote, part in zip(chunk_local, chunk_remote, range(3)):
        local.wait()
        remote.wait_send()
        other = pl.ds(pl.multiple_of(32 - core * 32, 32), 32)
        landed = rings[part].block((0, 0, 0)).at[other]
        to_partner(landed, landed, w_sems.at[1, part], w_sems.at[2, part]).wait_recv()

    def start(name):
        for copy in message(rings, name, send_sems, recv_sems):
            copy.start()

    def finish(name):
        for copy in message(rings, name, send_sems, recv_sems):
            copy.wait()

    start("own")
    wait_loads(("meta", 0))
    build_bias(meta_b, bias_b, NODES, NODES)
    build_bias(meta_l, bias_l, LIGHT, LIGHT)
    count_b, count_l = meta_b[16:17, :TILE], meta_l[16:17, :TILE]
    refs = (q_b, q_l, keys_b, values_b, keys_l, values_l, bias_b, bias_l, sinks, att)

    def att_half(side, kv):
        return att.at[:, pl.ds(pl.multiple_of(side * HALF + kv * 512, 512), 512)]

    def att_swap(kv):
        own = att_half(core, kv)
        return to_partner(own, own, att_send.at[kv], att_recv.at[kv])

    def per_pair(step, carry):
        kv = lax.div(step, 4)
        for when, waits, starts in PLAN:

            @pl.when(step == when)
            def _():
                for name in waits:
                    finish(name)
                for name in starts:
                    start(name)

        @pl.when(lax.rem(step, 4) == 0)
        def _():
            pair = lax.div(kv, 2)
            second = lax.rem(kv, 2) == 1
            wait_loads(("q", kv))
            pl.when(jnp.logical_not(second))(lambda: wait_loads(("kv", pair)))
            lanes = pl.ds(pl.multiple_of(pair * 128, 128), 128)
            prepare(
                kc_b[:, lanes], vc_b[:, lanes], kt_b[:, lanes], vt_b[:, lanes], meta_b[17:18, :],
                second, keys_b, values_b, NODES,
            )
            prepare(
                kc_l[:, lanes], vc_l[:, lanes], kt_l[:, lanes], vt_l[:, lanes], meta_l[17:18, :],
                second, keys_l, values_l, LIGHT,
            )

        attend_head_pair(step, core, refs, (count_b, count_l))

        @pl.when((lax.rem(step, 4) == 0) & (step > 0))
        def _():
            att_swap(kv - 1).start()

        return carry

    lax.fori_loop(0, 16, per_pair, 0)
    for name in ("back0", "back-", "back+"):
        finish(name)
    wait_sends()
    att_swap(3).start()
    finish("back2")
    for kv in range(4):
        att_swap(kv).wait_send()
        other = att_half(1 - core, kv)
        to_partner(other, other, att_send.at[kv], att_recv.at[kv]).wait_recv()

    def att_store(heavy):
        first, count = (0, NODES) if heavy else (NODES, LIGHT)
        return pltpu.make_async_copy(
            att.at[pl.ds(first, count)], att_hbm.at[pl.ds(0, count)], att_sem
        )

    by_role(lambda heavy: att_store(heavy).start())

    def proj_block(heavy, part):
        first, count = (0, NODES) if heavy else (NODES, LIGHT)
        return proj.at[part, pl.ds(first, count)]

    def proj_place(heavy, side, part):
        count = NODES if heavy else LIGHT
        columns = pl.ds(pl.multiple_of(side * COLS + part * PART, PART), PART)
        return proj_hbm.at[pl.ds(0, count), columns]

    def proj_copies(heavy, part):
        own = pltpu.make_async_copy(
            proj_block(heavy, part), proj_place(heavy, core, part), proj_sem.at[part]
        )
        sent = to_partner(
            proj_block(not heavy, part), proj_place(not heavy, core, part), proj_send.at[part],
            proj_recv.at[part],
        )
        return own, sent

    def start_proj(heavy, part):
        own, sent = proj_copies(heavy, part)
        sent.start()
        own.start()

    def finish_proj(heavy, part):
        own, sent = proj_copies(heavy, part)
        own.wait()
        sent.wait_send()
        landed = proj_place(heavy, 1 - core, part)
        to_partner(landed, landed, proj_send.at[part], proj_recv.at[part]).wait_recv()

    for part in range(3):

        def per_block(block, carry, part=part):
            rows = pl.ds(pl.multiple_of(block * 320, 64), 320)
            total = None
            for gx_at in range(8):
                term = jnp.dot(
                    att[rows, gx_at * 512 : gx_at * 512 + 512],
                    weights[part][gx_at // 2, gx_at % 2].reshape(512, PART),
                    preferred_element_type=F32,
                )
                total = term if total is None else total + term
            proj[part, rows, :] = total.astype(BF16)
            return carry

        lax.fori_loop(0, 2, per_block, 0)
        if part > 0:
            by_role(functools.partial(start_proj, part=part - 1))
    by_role(lambda heavy: att_store(heavy).wait())
    by_role(functools.partial(start_proj, part=2))
    for part in range(3):
        by_role(functools.partial(finish_proj, part=part))


def whole(sinks, *arrays):
    smem = pl.BlockSpec(memory_space=pltpu.SMEM)
    hbm = pl.BlockSpec(memory_space=pl.ANY)
    dma = pltpu.SemaphoreType.DMA

    def role(rows):
        return [
            pltpu.VMEM((rows, HALF), BF16),
            pltpu.VMEM((CACHE, 256), BF16),
            pltpu.VMEM((CACHE, 256), BF16),
            pltpu.VMEM((rows, 256), BF16),
            pltpu.VMEM((rows, 256), BF16),
            pltpu.VMEM((24, CACHE), jnp.int32),
        ]

    return pl.pallas_call(
        whole_kernel,
        out_shape=(
            jax.ShapeDtypeStruct((NODES, 2 * HALF), BF16),
            jax.ShapeDtypeStruct((NODES, 2 * COLS), BF16),
        ),
        in_specs=[smem] + [hbm] * len(arrays),
        out_specs=(hbm, hbm),
        scratch_shapes=role(NODES)
        + role(LIGHT)
        + [pltpu.VMEM((4, 2, 4, 2, 64, PART), BF16)] * 3
        + [
            pltpu.VMEM((NODES + LIGHT, 2 * HALF), BF16),
            pltpu.VMEM((3, NODES + LIGHT, PART), BF16),
            pltpu.VMEM((CACHE + NODES, 128), BF16),
            pltpu.VMEM((HD + SUMS, CACHE + NODES), BF16),
            pltpu.VMEM((CACHE + LIGHT, 128), BF16),
            pltpu.VMEM((HD + SUMS, CACHE + LIGHT), BF16),
            pltpu.VMEM((NODES, NODES), F32),
            pltpu.VMEM((LIGHT, LIGHT), F32),
            dma((len(NAMES), 3, 2)), dma((len(NAMES), 3, 2)),
            dma((13,)), dma((13,)), dma((13,)), dma((3, 3)),
            dma((4,)), dma((4,)), dma, dma((3,)), dma((3,)), dma((3,)),
        ],
        compiler_params=pltpu.CompilerParams(
            vmem_limit_bytes=60 * 1024 * 1024, collective_id=0, has_side_effects=True
        ),
        cost_estimate=pl.CostEstimate(
            flops=32 * (512 * 1536 + 128 * 1152) * 256, bytes_accessed=8 * 2**20, transcendentals=0
        ),
        name="whole",
    )(sinks, *arrays)


def on_device(
    q_nodes, k_cache, v_cache, k_tree, v_tree, anc_bits, node_count, cache_len, sinks, o_weight
):
    busy = lax.rem(lax.axis_index("gx") + lax.axis_index("core"), 2) == 0
    weight = jnp.pad(o_weight, ((0, 0), (0, 2 * COLS - D)))
    weight = jnp.transpose(weight.reshape(32, 2, 3, PART), (1, 2, 0, 3))
    bits = jnp.pad(anc_bits[0].T, ((0, 0), (0, CACHE - NODES)))
    ones = jnp.ones((1, CACHE), jnp.int32)
    meta = jnp.concatenate(
        [bits, ones * node_count[0], ones * cache_len[0], jnp.zeros((6, CACHE), jnp.int32)], axis=0
    )
    attended, projected = whole(
        sinks, q_nodes[0], k_cache[0], v_cache[0], k_tree[0], v_tree[0], meta, weight
    )
    kept = (jnp.arange(NODES) < jnp.where(busy, NODES, LIGHT))[:, None]

    def place(x):
        return jnp.where(kept, x, jnp.zeros_like(x))[None]

    return place(attended), place(projected[:, :D])


def solution(mesh):
    split = Mesh(mesh.devices.reshape(8, 8, 2), ("gx", "gyc", "core"))
    every = ("gx", "gyc", "core")
    placed = tuple([P(every)] * 8) + (P(), P(every))
    return jax.shard_map(
        on_device, mesh=split, in_specs=placed, out_specs=(P(every), P(every)), check_vma=False
    )
```

```python
import functools

import jax
import jax.numpy as jnp
from jax import lax
from jax.experimental import pallas as pl
from jax.experimental.pallas import tpu as pltpu
from jax.sharding import Mesh, PartitionSpec as P

HD = 64
NODES = 512
LIGHT = 128
CACHE = 1024
HALF = 2048
D = 2880
TILE = 256
SUMS = 16
EXP_SCALE = 0.125 * 1.4426950408889634
MASKED = -1.0e30
PART = 512
PART_COLS = 480
MESH = pl.DeviceIdType.MESH
WHERE = {"x": (2,), "y": (0,), "z": (1, 3)}
SIZES = (4, 2, 4, 2)
PLAN = (
    (1, ("own",), ("far", "l-", "l+", "f-", "f+")),
    (3, ("far",), ("l2", "f2")),
    (5, ("l0", "l-", "l+", "l2"), ("line2", "face-", "face+")),
    (6, ("f0", "f-", "f+", "f2"), ("back0",)),
    (7, ("line2",), ("face2",)),
    (11, ("face-", "face+"), ("back-", "back+")),
    (14, ("face2",), ("back2",)),
)
NAMES = (
    "own", "far", "l0", "l-", "l+", "l2", "line2", "f0", "f-", "f+", "f2", "face-", "face+",
    "face2", "back0", "back-", "back+", "back2",
)
LINES = {"0": 0, "-": -1, "+": 1, "2": 2}
F32 = jnp.float32
BF16 = jnp.bfloat16


def lane_ids(shape):
    return lax.broadcasted_iota(jnp.int32, shape, len(shape) - 1)


def row_ids(shape):
    return lax.broadcasted_iota(jnp.int32, shape, len(shape) - 2)


def build_bias(bits_ref, bias_ref, keys, nodes):
    shift = row_ids((32, nodes))
    for word in range(keys // 32):
        row = jnp.broadcast_to(bits_ref[word : word + 1, :nodes], (32, nodes))
        bit = jnp.bitwise_and(lax.shift_right_logical(row, shift), 1)
        bias_ref[word * 32 : word * 32 + 32, :] = jnp.where(bit > 0, 0.0, MASKED)


def spread_keys(pair, second):
    wide = pair.astype(F32)
    turned = pltpu.roll(wide, HD, 1)
    take_own = (lane_ids(wide.shape) < HD) == jnp.logical_not(second)
    return jnp.where(take_own, wide, turned)


def turn_values(pair, second):
    turned = pair.astype(F32).T
    return jnp.where(second, turned[HD:], turned[:HD])


def prepare(k_cache, v_cache, k_tree, v_tree, length, second, keys_ref, values_ref, tree):
    keys = spread_keys(k_cache, second)
    keys_ref[pl.ds(0, CACHE), :] = jnp.where(row_ids(keys.shape) < length[:, :128], keys, 0.0).astype(BF16)
    keys_ref[pl.ds(CACHE, tree), :] = spread_keys(k_tree, second).astype(BF16)
    values = turn_values(v_cache, second)
    live = lane_ids(values.shape) < length
    values_ref[pl.ds(0, HD), pl.ds(0, CACHE)] = jnp.where(live, values, 0.0).astype(BF16)
    live = lane_ids((SUMS, CACHE)) < length
    values_ref[pl.ds(HD, SUMS), pl.ds(0, CACHE)] = jnp.where(live, 1.0, 0.0).astype(BF16)
    values_ref[pl.ds(0, HD), pl.ds(CACHE, tree)] = turn_values(v_tree, second).astype(BF16)
    values_ref[pl.ds(HD, SUMS), pl.ds(CACHE, tree)] = jnp.ones((SUMS, tree), BF16)


def contract_last(a, b):
    return lax.dot_general(a, b, (((1,), (1,)), ((), ())), preferred_element_type=F32)


def fold_max(scores):
    rows = scores.shape[0]
    return jnp.max(scores.reshape(rows // 8, 8, TILE), axis=0)


class Unit:
    def __init__(self, keys, values, queries, bias, tree, sink, node_ok, scores):
        self.keys, self.values, self.queries, self.bias = keys, values, queries, bias
        self.sink, self.node_ok, self.scores = sink, node_ok, scores
        self.chunks = [(at, TILE) for at in range(0, CACHE, TILE)]
        self.chunks += [(CACHE + at, min(TILE, tree)) for at in range(0, tree, TILE)]
        self.peak = None
        self.total = None

    def score(self, number):
        at, count = self.chunks[number]
        scores = contract_last(self.keys[pl.ds(at, count), :], self.queries)
        if at >= CACHE:
            scores = scores + self.bias(at - CACHE, count)
        self.scores[pl.ds(at, count), :] = scores
        peak = fold_max(scores)
        self.peak = peak if self.peak is None else jnp.maximum(self.peak, peak)

    def settle(self):
        self.row_max = jnp.maximum(jnp.max(self.peak, axis=0, keepdims=True), self.sink)

    def weigh(self, number):
        at, count = self.chunks[number]
        weights = jnp.exp2((self.scores[pl.ds(at, count), :] - self.row_max) * EXP_SCALE)
        term = jnp.dot(
            self.values[:, pl.ds(at, count)], weights.astype(BF16), preferred_element_type=F32
        )
        self.total = term if self.total is None else self.total + term

    def result(self):
        denominator = self.total[HD : HD + 1] + jnp.exp2((self.sink - self.row_max) * EXP_SCALE)
        return self.total[:HD] * jnp.where(self.node_ok, 1.0 / denominator, 0.0)


def attend_head_pair(pair, core, refs, counts):
    (q_busy, q_light, keys_b, values_b, keys_l, values_l, bias_b, bias_l, sinks, att, scores) = refs
    count_b, count_l = counts
    lanes = pl.ds(pl.multiple_of(pair * 128, 128), 128)
    out_lanes = pl.ds(pl.multiple_of(core * HALF + pair * 128, 128), 128)
    first_head = core * 32
    sink_even = sinks[first_head + 2 * pair] * 8.0
    sink_odd = sinks[first_head + 2 * pair + 1] * 8.0
    columns = lane_ids((1, TILE))
    units = []
    for tile in range(NODES // TILE):
        rows = pl.ds(tile * TILE, TILE)
        for odd, sink in enumerate((sink_even, sink_odd)):

            def queries(rows=rows, odd=odd):
                both = q_busy[rows, lanes]
                return jnp.where((lane_ids(both.shape) < HD) == (odd == 0), both, jnp.zeros_like(both))

            units.append(
                Unit(
                    keys_b, values_b, queries(),
                    lambda at, count, rows=rows: bias_b[pl.ds(at, count), rows],
                    (tile + 1) * TILE, sink, columns + tile * TILE < count_b,
                    scores.at[len(units) % 2],
                )
            )
    both = q_light[:, lanes]
    left = lane_ids(both.shape) < HD
    zero = jnp.zeros_like(both)
    both = jnp.concatenate([jnp.where(left, both, zero), jnp.where(left, zero, both)], axis=0)
    units.append(
        Unit(
            keys_l, values_l, both,
            lambda at, count: jnp.concatenate([bias_l[...], bias_l[...]], axis=1), LIGHT,
            jnp.where(columns < LIGHT, sink_even, sink_odd),
            jnp.where(columns < LIGHT, columns, columns - LIGHT) < count_l,
            scores.at[len(units) % 2],
        )
    )
    results = []
    for number in range(len(units) + 1):
        ahead = units[number] if number < len(units) else None
        behind = units[number - 1] if number > 0 else None
        for chunk in range(6):
            if ahead is not None and chunk < len(ahead.chunks):
                ahead.score(chunk)
            if behind is not None and chunk < len(behind.chunks):
                behind.weigh(chunk)
        if behind is not None:
            results.append(behind.result())
        if ahead is not None:
            ahead.settle()
        if number in (2, 4):
            rows = pl.ds((number // 2 - 1) * TILE, TILE)
            att[rows, out_lanes] = jnp.concatenate(results[-2:], axis=0).T.astype(BF16)
    result = results[-1]
    stacked = jnp.concatenate([result[:, :LIGHT], result[:, LIGHT:]], axis=0)
    att[pl.ds(NODES, LIGHT), out_lanes] = stacked.T.astype(BF16)


class Ring:
    def __init__(self, order, place, core, weights):
        self.order, self.place, self.core, self.weights = order, place, core, weights

    def moved(self, dim, by):
        return lax.rem(self.place[dim] + 4 + by, 4)

    def device(self, dim, by):
        at = dict(self.place)
        at[dim] = self.moved(dim, by)
        x, y, z = at["x"], at["y"], at["z"]
        return (y * 2 + lax.div(z, 2), x * 2 + lax.rem(z, 2), self.core)

    def block(self, offsets, whole=False, half=None):
        at = {dim: self.moved(dim, by) for dim, by in zip(self.order, offsets)}
        index = [at["y"], lax.div(at["z"], 2), at["x"], lax.rem(at["z"], 2), slice(None)]
        axes = WHERE[self.order[0]] if whole else (4,)
        if whole:
            for axis in axes:
                index[axis] = slice(None)
        if half is not None:
            size = (SIZES[axes[0]] if whole else 64) // 2
            index[axes[0]] = pl.ds(half * size, size)
        return self.weights.at[tuple(index)]

    def send(self, name, side):
        by = (1, -1)[side]
        if name == "own":
            return 0, self.block((0, 0, 0))
        if name == "far":
            return 0, self.block((-by, 0, 0), half=side)
        if name == "line2":
            return 1, self.block((0, -by, 0), whole=True, half=side)
        line = LINES[name[-1]]
        if len(name) == 2:
            return {"l": 1, "f": 2}[name[0]], self.block((line, 0, 0))
        if name.startswith("face"):
            return 2, self.block((0, line, 0), whole=True)
        return 2, self.block((0, line, -by), whole=True, half=side)


def message(rings, name, send_sems, recv_sems):
    number = NAMES.index(name)
    copies = []
    for part, ring in enumerate(rings):
        for side in range(2):
            axis, block = ring.send(name, side)
            copies.append(
                pltpu.make_async_remote_copy(
                    src_ref=block, dst_ref=block,
                    send_sem=send_sems.at[number, part, side],
                    recv_sem=recv_sems.at[number, part, side],
                    device_id=ring.device(ring.order[axis], (1, -1)[side]),
                    device_id_type=MESH,
                )
            )
    return copies


def whole_kernel(
    sinks, q_hbm, kc_hbm, vc_hbm, kt_hbm, vt_hbm, meta_hbm, w_hbm, att_hbm, proj_hbm,
    q_b, kc_b, vc_b, kt_b, vt_b, meta_b, q_l, kc_l, vc_l, kt_l, vt_l, meta_l,
    weights_0, weights_1, weights_2, att, proj, partial, scores, keys_b, values_b, keys_l, values_l, bias_b, bias_l,
    send_sems, recv_sems, load_sems, load_send, load_recv, w_sems, att_send, att_recv, att_sem,
    proj_send, proj_recv, proj_sem,
):
    gx, gyc, core = lax.axis_index("gx"), lax.axis_index("gyc"), lax.axis_index("core")
    partner = (gx, gyc, 1 - core)
    busy = lax.rem(gx + core, 2) == 0
    place = {
        "x": lax.div(gyc, 2), "y": lax.div(gx, 2), "z": lax.rem(gx, 2) * 2 + lax.rem(gyc, 2)
    }
    weights = (weights_0, weights_1, weights_2)
    rings = [Ring(order, place, core, w) for order, w in zip(("xyz", "yzx", "zxy"), weights)]

    def by_role(run):
        pl.when(busy)(lambda: run(True))
        pl.when(jnp.logical_not(busy))(lambda: run(False))

    def to_partner(source, target, send, recv):
        return pltpu.make_async_remote_copy(
            src_ref=source, dst_ref=target, send_sem=send, recv_sem=recv, device_id=partner,
            device_id_type=MESH,
        )

    def load_pairs(heavy, piece, half):
        rows, q, kc, vc, kt, vt, meta = (
            (NODES, q_b, kc_b, vc_b, kt_b, vt_b, meta_b)
            if heavy
            else (LIGHT, q_l, kc_l, vc_l, kt_l, vt_l, meta_l)
        )
        if piece[0] == "q":
            return [
                (
                    q_hbm.at[pl.ds(0, rows), pl.ds(half * HALF + piece[1] * 512, 512)],
                    q.at[:, pl.ds(pl.multiple_of(piece[1] * 512, 512), 512)],
                )
            ]
        if piece[0] == "meta":
            return [(meta_hbm, meta)]
        source = pl.ds(half * 256 + piece[1] * 128, 128)
        target = pl.ds(pl.multiple_of(piece[1] * 128, 128), 128)
        return [
            (kc_hbm.at[:, source], kc.at[:, target]),
            (vc_hbm.at[:, source], vc.at[:, target]),
            (kt_hbm.at[pl.ds(0, rows), source], kt.at[:, target]),
            (vt_hbm.at[pl.ds(0, rows), source], vt.at[:, target]),
        ]

    def slot(piece):
        return {"meta": 0, "q": 1, "kv": 5}[piece[0]] + piece[1] * (4 if piece[0] == "kv" else 1)

    def local_loads(heavy, piece):
        pairs = load_pairs(heavy, piece, core)
        return [
            pltpu.make_async_copy(a, b, load_sems.at[slot(piece) + i])
            for i, (a, b) in enumerate(pairs)
        ]

    def remote_loads(heavy, piece):
        pairs = load_pairs(heavy, piece, 1 - core)
        return [
            to_partner(a, b, load_send.at[slot(piece) + i], load_recv.at[slot(piece) + i])
            for i, (a, b) in enumerate(pairs)
        ]

    def start_loads(heavy):
        pieces = [("meta", 0), ("kv", 0)] + [("q", kv) for kv in range(4)]
        pieces.insert(5, ("kv", 1))
        for piece in pieces:
            for copy in remote_loads(heavy, piece) + local_loads(heavy, piece):
                copy.start()

    def wait_loads(piece):
        def run(heavy):
            for copy in local_loads(heavy, piece):
                copy.wait()
            for copy in remote_loads(not heavy, piece):
                copy.wait_recv()

        by_role(run)

    def wait_sends():
        def run(heavy):
            for piece in [("meta", 0)] + [("q", kv) for kv in range(4)] + [("kv", 0), ("kv", 1)]:
                for copy in remote_loads(heavy, piece):
                    copy.wait_send()

        by_role(run)

    barrier = pltpu.get_barrier_semaphore()
    for dim in "xyz":
        for by in (1, -1):
            pl.semaphore_signal(
                barrier, inc=1, device_id=rings[0].device(dim, by), device_id_type=MESH
            )
    pl.semaphore_signal(barrier, inc=1, device_id=partner, device_id_type=MESH)
    pl.semaphore_wait(barrier, 7)

    rows = pl.ds(pl.multiple_of(core * 32, 32), 32)
    chunk_local, chunk_remote = [], []
    for part, ring in enumerate(rings):
        target = ring.block((0, 0, 0)).at[rows]
        chunk_local.append(
            pltpu.make_async_copy(w_hbm.at[core, part], target, w_sems.at[0, part])
        )
        chunk_remote.append(
            to_partner(w_hbm.at[1 - core, part], target, w_sems.at[1, part], w_sems.at[2, part])
        )
    for copy in chunk_remote + chunk_local:
        copy.start()
    by_role(start_loads)
    for local, remote, part in zip(chunk_local, chunk_remote, range(3)):
        local.wait()
        remote.wait_send()
        other = pl.ds(pl.multiple_of(32 - core * 32, 32), 32)
        landed = rings[part].block((0, 0, 0)).at[other]
        to_partner(landed, landed, w_sems.at[1, part], w_sems.at[2, part]).wait_recv()

    def start(name):
        for copy in message(rings, name, send_sems, recv_sems):
            copy.start()

    def finish(name):
        for copy in message(rings, name, send_sems, recv_sems):
            copy.wait()

    for name in ("own", "l0", "f0"):
        start(name)
    wait_loads(("meta", 0))
    build_bias(meta_b, bias_b, NODES, NODES)
    build_bias(meta_l, bias_l, LIGHT, LIGHT)
    count_b, count_l = meta_b[16:17, :TILE], meta_l[16:17, :TILE]
    refs = (q_b, q_l, keys_b, values_b, keys_l, values_l, bias_b, bias_l, sinks, att, scores)

    def wide(meta):
        return jnp.concatenate([meta[17:18, :], meta[17:18, :]], axis=1)

    def att_half(side, kv):
        return att.at[:, pl.ds(pl.multiple_of(side * HALF + kv * 512, 512), 512)]

    def att_swap(kv):
        own = att_half(core, kv)
        return to_partner(own, own, att_send.at[kv], att_recv.at[kv])

    def per_pair(step, carry):
        kv = lax.div(step, 4)
        for when, waits, starts in PLAN:

            @pl.when(step == when)
            def _():
                for name in waits:
                    finish(name)
                for name in starts:
                    start(name)

        @pl.when(lax.rem(step, 4) == 0)
        def _():
            pair = lax.div(kv, 2)
            second = lax.rem(kv, 2) == 1
            wait_loads(("q", kv))
            pl.when(jnp.logical_not(second))(lambda: wait_loads(("kv", pair)))
            lanes = pl.ds(pl.multiple_of(pair * 128, 128), 128)
            prepare(
                kc_b[:, lanes], vc_b[:, lanes], kt_b[:, lanes], vt_b[:, lanes], wide(meta_b),
                second, keys_b, values_b, NODES,
            )
            prepare(
                kc_l[:, lanes], vc_l[:, lanes], kt_l[:, lanes], vt_l[:, lanes], wide(meta_l),
                second, keys_l, values_l, LIGHT,
            )

        attend_head_pair(step, core, refs, (count_b, count_l))

        @pl.when((lax.rem(step, 4) == 0) & (step > 0))
        def _():
            att_swap(kv - 1).start()

        return carry

    lax.fori_loop(0, 16, per_pair, 0)
    wait_sends()
    att_swap(3).start()
    for kv in range(4):
        att_swap(kv).wait_send()
        other = att_half(1 - core, kv)
        to_partner(other, other, att_send.at[kv], att_recv.at[kv]).wait_recv()

    def att_store(heavy):
        first, count = (0, NODES) if heavy else (NODES, LIGHT)
        return pltpu.make_async_copy(
            att.at[pl.ds(first, count)], att_hbm.at[pl.ds(0, count)], att_sem
        )

    by_role(lambda heavy: att_store(heavy).start())

    def proj_block(heavy, part):
        first, count = (0, NODES) if heavy else (NODES, LIGHT)
        return proj.at[part, pl.ds(0, PART_COLS), pl.ds(first, count)]

    def proj_place(heavy, side, part):
        count = NODES if heavy else LIGHT
        rows = pl.ds(pl.multiple_of((side * 3 + part) * PART_COLS, 32), PART_COLS)
        return proj_hbm.at[rows, pl.ds(0, count)]

    def proj_copies(heavy, part):
        own = pltpu.make_async_copy(
            proj_block(heavy, part), proj_place(heavy, core, part), proj_sem.at[part]
        )
        sent = to_partner(
            proj_block(not heavy, part), proj_place(not heavy, core, part), proj_send.at[part],
            proj_recv.at[part],
        )
        return own, sent

    def start_proj(heavy, part):
        own, sent = proj_copies(heavy, part)
        sent.start()
        own.start()

    def finish_proj(heavy, part):
        own, sent = proj_copies(heavy, part)
        own.wait()
        sent.wait_send()
        landed = proj_place(heavy, 1 - core, part)
        to_partner(landed, landed, proj_send.at[part], proj_recv.at[part]).wait_recv()

    def lanes_of(rows, first, count):
        return att[rows, pl.ds(pl.multiple_of(first, 128), count)]

    def terms(part, rows, last):
        ring = rings[part]
        pairs = []
        if part == 0:
            z_hi = lax.div(place["z"], 2)
            z_hi = 1 - z_hi if last else z_hi
            for y in range(4):
                pairs.append(
                    (lanes_of(rows, (2 * y + z_hi) * 512, 512), weights_0[y, z_hi].reshape(512, PART))
                )
        else:
            for by in (2,) if last else (0, 1, -1):
                at = ring.moved(ring.order[2], by)
                if part == 1:
                    left = [lanes_of(rows, g * 512 + at * 128, 128) for g in range(8)]
                    right = weights_1[:, :, at].reshape(1024, PART)
                    pairs.append((jnp.concatenate(left, axis=1), right))
                else:
                    pairs.append((lanes_of(rows, at * 1024, 1024), weights_2[at].reshape(1024, PART)))
        total = None
        for left, right in pairs:
            term = jnp.dot(left, right, preferred_element_type=F32)
            total = term if total is None else total + term
        return total

    row_blocks = (pl.ds(0, 384), pl.ds(384, 256))
    for part in range(3):
        for rows in row_blocks:
            partial[part, rows, :] = terms(part, rows, False)
    for name in ("back0", "back-", "back+", "back2"):
        finish(name)
    for part in range(3):
        for rows in row_blocks:
            total = partial[part, rows, :] + terms(part, rows, True)
            proj[part, :, rows] = total.T.astype(BF16)
        if part > 0:
            by_role(functools.partial(start_proj, part=part - 1))
    by_role(lambda heavy: att_store(heavy).wait())
    by_role(functools.partial(start_proj, part=2))
    for part in range(3):
        by_role(functools.partial(finish_proj, part=part))


def whole(sinks, *arrays):
    smem = pl.BlockSpec(memory_space=pltpu.SMEM)
    hbm = pl.BlockSpec(memory_space=pl.ANY)
    dma = pltpu.SemaphoreType.DMA

    def role(rows):
        return [
            pltpu.VMEM((rows, HALF), BF16),
            pltpu.VMEM((CACHE, 256), BF16),
            pltpu.VMEM((CACHE, 256), BF16),
            pltpu.VMEM((rows, 256), BF16),
            pltpu.VMEM((rows, 256), BF16),
            pltpu.VMEM((24, NODES), jnp.int32),
        ]

    return pl.pallas_call(
        whole_kernel,
        out_shape=(
            jax.ShapeDtypeStruct((NODES, 2 * HALF), BF16),
            jax.ShapeDtypeStruct((D, NODES), BF16),
        ),
        in_specs=[smem] + [hbm] * len(arrays),
        out_specs=(hbm, hbm),
        scratch_shapes=role(NODES)
        + role(LIGHT)
        + [pltpu.VMEM((4, 2, 4, 2, 64, PART), BF16)] * 3
        + [
            pltpu.VMEM((NODES + LIGHT, 2 * HALF), BF16),
            pltpu.VMEM((3, PART, NODES + LIGHT), BF16),
            pltpu.VMEM((3, NODES + LIGHT, PART), F32),
            pltpu.VMEM((2, CACHE + NODES, TILE), F32),
            pltpu.VMEM((CACHE + NODES, 128), BF16),
            pltpu.VMEM((HD + SUMS, CACHE + NODES), BF16),
            pltpu.VMEM((CACHE + LIGHT, 128), BF16),
            pltpu.VMEM((HD + SUMS, CACHE + LIGHT), BF16),
            pltpu.VMEM((NODES, NODES), F32),
            pltpu.VMEM((LIGHT, LIGHT), F32),
            dma((len(NAMES), 3, 2)), dma((len(NAMES), 3, 2)),
            dma((13,)), dma((13,)), dma((13,)), dma((3, 3)),
            dma((4,)), dma((4,)), dma, dma((3,)), dma((3,)), dma((3,)),
        ],
        compiler_params=pltpu.CompilerParams(
            vmem_limit_bytes=60 * 1024 * 1024, collective_id=0, has_side_effects=True
        ),
        cost_estimate=pl.CostEstimate(
            flops=32 * (512 * 1536 + 128 * 1152) * 256, bytes_accessed=8 * 2**20, transcendentals=0
        ),
        name="whole",
    )(sinks, *arrays)


def on_device(
    q_nodes, k_cache, v_cache, k_tree, v_tree, anc_bits, node_count, cache_len, sinks, o_weight
):
    busy = lax.rem(lax.axis_index("gx") + lax.axis_index("core"), 2) == 0
    weight = jnp.transpose(o_weight.reshape(32, 2, 3, PART_COLS), (1, 2, 0, 3))
    weight = jnp.pad(weight, ((0, 0), (0, 0), (0, 0), (0, PART - PART_COLS)))
    bits = jnp.pad(anc_bits[0].T, ((0, 8), (0, 0)))
    row = lax.broadcasted_iota(jnp.int32, bits.shape, 0)
    meta = jnp.where(row == 16, node_count[0], jnp.where(row == 17, cache_len[0], bits))
    attended, projected = whole(
        sinks, q_nodes[0], k_cache[0], v_cache[0], k_tree[0], v_tree[0], meta, weight
    )
    kept = jnp.arange(NODES) < jnp.where(busy, NODES, LIGHT)
    attended = jnp.where(kept[:, None], attended, jnp.zeros_like(attended))
    projected = jnp.where(kept[None, :], projected, jnp.zeros_like(projected))
    return attended[None], projected.T[None]


def solution(mesh):
    split = Mesh(mesh.devices.reshape(8, 8, 2), ("gx", "gyc", "core"))
    every = ("gx", "gyc", "core")
    placed = tuple([P(every)] * 8) + (P(), P(every))
    return jax.shard_map(
        on_device, mesh=split, in_specs=placed, out_specs=(P(every), P(every)), check_vma=False
    )
```

```python
import functools

import jax
import jax.numpy as jnp
from jax import lax
from jax.experimental import pallas as pl
from jax.experimental.pallas import tpu as pltpu
from jax.sharding import Mesh, PartitionSpec as P

HD = 64
NODES = 512
LIGHT = 128
KEEP = 4
CACHE = 1024
HALF = 2048
D = 2880
TILE = 256
SUMS = 16
EXP_SCALE = 0.125 * 1.4426950408889634
MASKED = -1.0e30
PART = 512
PART_COLS = 480
MESH = pl.DeviceIdType.MESH
WHERE = {"x": (2,), "y": (0,), "z": (1, 3)}
SIZES = (4, 2, 4, 2)
PLAN = (
    (1, ("far",), ("l2", "f2")),
    (2, ("l0", "l-", "l+", "l2"), ("line2", "face-", "face+")),
    (3, ("line2", "f0", "f-", "f+", "f2"), ("face2", "back0")),
    (5, ("face-", "face+"), ("back-", "back+")),
    (7, ("face2",), ("back2",)),
)
NAMES = (
    "own", "far", "l0", "l-", "l+", "l2", "line2", "f0", "f-", "f+", "f2", "face-", "face+",
    "face2", "back0", "back-", "back+", "back2",
)
LINES = {"0": 0, "-": -1, "+": 1, "2": 2}
F32 = jnp.float32
BF16 = jnp.bfloat16


def lane_ids(shape):
    return lax.broadcasted_iota(jnp.int32, shape, len(shape) - 1)


def row_ids(shape):
    return lax.broadcasted_iota(jnp.int32, shape, len(shape) - 2)


def build_bias(bits_ref, bias_ref, keys, nodes):
    shift = row_ids((32, nodes))
    for word in range(keys // 32):
        row = jnp.broadcast_to(bits_ref[word : word + 1, :nodes], (32, nodes))
        bit = jnp.bitwise_and(lax.shift_right_logical(row, shift), 1)
        bias_ref[word * 32 : word * 32 + 32, :] = jnp.where(bit > 0, 0.0, MASKED)


def spread_keys(pair, second):
    wide = pair.astype(F32)
    turned = pltpu.roll(wide, HD, 1)
    take_own = (lane_ids(wide.shape) < HD) == jnp.logical_not(second)
    return jnp.where(take_own, wide, turned)


def turn_values(pair, second):
    turned = pair.astype(F32).T
    return jnp.where(second, turned[HD:], turned[:HD])


def prepare(k_cache, v_cache, k_tree, v_tree, length, second, keys_ref, values_ref, tree):
    keys = spread_keys(k_cache, second)
    keys_ref[pl.ds(0, CACHE), :] = jnp.where(row_ids(keys.shape) < length[:, :128], keys, 0.0).astype(BF16)
    keys_ref[pl.ds(CACHE, tree), :] = spread_keys(k_tree, second).astype(BF16)
    values = turn_values(v_cache, second)
    live = lane_ids(values.shape) < length
    values_ref[pl.ds(0, HD), pl.ds(0, CACHE)] = jnp.where(live, values, 0.0).astype(BF16)
    live = lane_ids((SUMS, CACHE)) < length
    values_ref[pl.ds(HD, SUMS), pl.ds(0, CACHE)] = jnp.where(live, 1.0, 0.0).astype(BF16)
    values_ref[pl.ds(0, HD), pl.ds(CACHE, tree)] = turn_values(v_tree, second).astype(BF16)
    values_ref[pl.ds(HD, SUMS), pl.ds(CACHE, tree)] = jnp.ones((SUMS, tree), BF16)


def contract_last(a, b):
    return lax.dot_general(a, b, (((1,), (1,)), ((), ())), preferred_element_type=F32)


def fold_max(scores):
    rows = scores.shape[0]
    return jnp.max(scores.reshape(rows // 8, 8, TILE), axis=0)


class Unit:
    def __init__(self, keys, values, queries, bias, tree, sink, node_ok, scores):
        self.keys, self.values, self.queries, self.bias = keys, values, queries, bias
        self.sink, self.node_ok, self.scores = sink, node_ok, scores
        self.chunks = [(at, TILE) for at in range(0, CACHE, TILE)]
        self.chunks += [(CACHE + at, min(TILE, tree)) for at in range(0, tree, TILE)]
        self.peak = None
        self.total = None

    def score(self, number):
        at, count = self.chunks[number]
        scores = contract_last(self.keys[pl.ds(at, count), :], self.queries)
        if at >= CACHE:
            scores = scores + self.bias(at - CACHE, count)
        self.scores[pl.ds(at, count), :] = scores
        peak = fold_max(scores)
        self.peak = peak if self.peak is None else jnp.maximum(self.peak, peak)

    def settle(self):
        self.row_max = jnp.maximum(jnp.max(self.peak, axis=0, keepdims=True), self.sink)

    def weigh(self, number):
        at, count = self.chunks[number]
        weights = jnp.exp2((self.scores[pl.ds(at, count), :] - self.row_max) * EXP_SCALE)
        term = jnp.dot(
            self.values[:, pl.ds(at, count)], weights.astype(BF16), preferred_element_type=F32
        )
        self.total = term if self.total is None else self.total + term

    def result(self):
        denominator = self.total[HD : HD + 1] + jnp.exp2((self.sink - self.row_max) * EXP_SCALE)
        return self.total[:HD] * jnp.where(self.node_ok, 1.0 / denominator, 0.0)


def attend_pairs(step, core, refs, counts):
    (q_busy, q_light, keys_b, values_b, keys_l, values_l, bias_b, bias_l, sinks, att, scores) = refs
    count_b, count_l = counts
    columns = lane_ids((1, TILE))
    units, outputs = [], {}
    for inner in range(2):
        pair = 2 * step + inner
        lanes = pl.ds(pl.multiple_of(pair * 128, 128), 128)
        out_lanes = pl.ds(pl.multiple_of(core * HALF + pair * 128, 128), 128)
        sink_even = sinks[core * 32 + 2 * pair] * 8.0
        sink_odd = sinks[core * 32 + 2 * pair + 1] * 8.0
        for tile in range(NODES // TILE):
            rows = pl.ds(tile * TILE, TILE)
            for odd, sink in enumerate((sink_even, sink_odd)):
                both = q_busy[rows, lanes]
                own = (lane_ids(both.shape) < HD) == (odd == 0)
                units.append(
                    Unit(
                        keys_b, values_b, jnp.where(own, both, jnp.zeros_like(both)),
                        lambda at, count, rows=rows: bias_b[pl.ds(at, count), rows],
                        (tile + 1) * TILE, sink, columns + tile * TILE < count_b,
                        scores.at[len(units) % 3],
                    )
                )
            outputs[len(units) - 1] = (rows, out_lanes)
        both = q_light[:, lanes]
        left = lane_ids(both.shape) < HD
        zero = jnp.zeros_like(both)
        both = jnp.concatenate([jnp.where(left, both, zero), jnp.where(left, zero, both)], axis=0)
        units.append(
            Unit(
                keys_l, values_l, both,
                lambda at, count: jnp.concatenate([bias_l[...], bias_l[...]], axis=1), LIGHT,
                jnp.where(columns < LIGHT, sink_even, sink_odd),
                jnp.where(columns < LIGHT, columns, columns - LIGHT) < count_l,
                scores.at[len(units) % 3],
            )
        )
        outputs[len(units) - 1] = (None, out_lanes)
    results = []
    for number in range(len(units) + 2):
        ahead = units[number] if number < len(units) else None
        behind = units[number - 2] if number >= 2 else None
        for chunk in range(6):
            if ahead is not None and chunk < len(ahead.chunks):
                ahead.score(chunk)
            if behind is not None and chunk < len(behind.chunks):
                behind.weigh(chunk)
        if behind is not None:
            results.append(behind.result())
        if ahead is not None:
            ahead.settle()
        if number - 2 in outputs:
            rows, out_lanes = outputs[number - 2]
            if rows is None:
                rows = pl.ds(NODES, LIGHT)
                pieces = [results[-1][:, :LIGHT], results[-1][:, LIGHT:]]
            else:
                pieces = results[-2:]
            att[rows, out_lanes] = jnp.concatenate(pieces, axis=0).T.astype(BF16)


class Ring:
    def __init__(self, order, place, core, weights):
        self.order, self.place, self.core, self.weights = order, place, core, weights

    def moved(self, dim, by):
        return lax.rem(self.place[dim] + 4 + by, 4)

    def device(self, dim, by):
        at = dict(self.place)
        at[dim] = self.moved(dim, by)
        x, y, z = at["x"], at["y"], at["z"]
        return (y * 2 + lax.div(z, 2), x * 2 + lax.rem(z, 2), self.core)

    def block(self, offsets, whole=False, half=None):
        at = {dim: self.moved(dim, by) for dim, by in zip(self.order, offsets)}
        index = [at["y"], lax.div(at["z"], 2), at["x"], lax.rem(at["z"], 2), slice(None)]
        axes = WHERE[self.order[0]] if whole else (4,)
        if whole:
            for axis in axes:
                index[axis] = slice(None)
        if half is not None:
            size = (SIZES[axes[0]] if whole else 64) // 2
            index[axes[0]] = pl.ds(half * size, size)
        return self.weights.at[tuple(index)]

    def send(self, name, side):
        by = (1, -1)[side]
        if name == "own":
            return 0, self.block((0, 0, 0))
        if name == "far":
            return 0, self.block((-by, 0, 0), half=side)
        if name == "line2":
            return 1, self.block((0, -by, 0), whole=True, half=side)
        line = LINES[name[-1]]
        if len(name) == 2:
            return {"l": 1, "f": 2}[name[0]], self.block((line, 0, 0))
        if name.startswith("face"):
            return 2, self.block((0, line, 0), whole=True)
        return 2, self.block((0, line, -by), whole=True, half=side)


def message(rings, name, send_sems, recv_sems):
    number = NAMES.index(name)
    copies = []
    for part, ring in enumerate(rings):
        for side in range(2):
            axis, block = ring.send(name, side)
            copies.append(
                pltpu.make_async_remote_copy(
                    src_ref=block, dst_ref=block,
                    send_sem=send_sems.at[number, part, side],
                    recv_sem=recv_sems.at[number, part, side],
                    device_id=ring.device(ring.order[axis], (1, -1)[side]),
                    device_id_type=MESH,
                )
            )
    return copies


def whole_kernel(
    sinks, q_hbm, kc_hbm, vc_hbm, kt_hbm, vt_hbm, bits_hbm, count_hbm, w_hbm, att_hbm, proj_hbm,
    q_b, kc_b, vc_b, kt_b, vt_b, meta_b, q_l, kc_l, vc_l, kt_l, vt_l, meta_l,
    weights_0, weights_1, weights_2, att, proj, partial, w_raw, w_split, scores, keys_b, values_b, keys_l, values_l, bias_b, bias_l,
    send_sems, recv_sems, load_sems, load_send, load_recv, w_sems, att_send, att_recv, att_sem,
    proj_send, proj_recv, proj_sem,
):
    gx, gyc, core = lax.axis_index("gx"), lax.axis_index("gyc"), lax.axis_index("core")
    partner = (gx, gyc, 1 - core)
    busy = lax.rem(gx + core, 2) == 0
    place = {
        "x": lax.div(gyc, 2), "y": lax.div(gx, 2), "z": lax.rem(gx, 2) * 2 + lax.rem(gyc, 2)
    }
    weights = (weights_0, weights_1, weights_2)
    rings = [Ring(order, place, core, w) for order, w in zip(("xyz", "yzx", "zxy"), weights)]

    def by_role(run):
        pl.when(busy)(lambda: run(True))
        pl.when(jnp.logical_not(busy))(lambda: run(False))

    def to_partner(source, target, send, recv):
        return pltpu.make_async_remote_copy(
            src_ref=source, dst_ref=target, send_sem=send, recv_sem=recv, device_id=partner,
            device_id_type=MESH,
        )

    def load_pairs(heavy, piece, half):
        rows, q, kc, vc, kt, vt, meta = (
            (NODES, q_b, kc_b, vc_b, kt_b, vt_b, meta_b)
            if heavy
            else (LIGHT, q_l, kc_l, vc_l, kt_l, vt_l, meta_l)
        )
        if piece[0] == "q":
            return [
                (
                    q_hbm.at[pl.ds(0, rows), pl.ds(half * HALF + piece[1] * 512, 512)],
                    q.at[:, pl.ds(pl.multiple_of(piece[1] * 512, 512), 512)],
                )
            ]
        if piece[0] == "meta":
            return [(bits_hbm, meta.at[pl.ds(0, 16)]), (count_hbm, meta.at[pl.ds(16, 8)])]
        source = pl.ds(half * 256 + piece[1] * 128, 128)
        target = pl.ds(pl.multiple_of(piece[1] * 128, 128), 128)
        return [
            (kc_hbm.at[:, source], kc.at[:, target]),
            (vc_hbm.at[:, source], vc.at[:, target]),
            (kt_hbm.at[pl.ds(0, rows), source], kt.at[:, target]),
            (vt_hbm.at[pl.ds(0, rows), source], vt.at[:, target]),
        ]

    def slot(piece):
        return {"meta": 0, "q": 2, "kv": 6}[piece[0]] + piece[1] * (4 if piece[0] == "kv" else 1)

    def local_loads(heavy, piece):
        pairs = load_pairs(heavy, piece, core)
        return [
            pltpu.make_async_copy(a, b, load_sems.at[slot(piece) + i])
            for i, (a, b) in enumerate(pairs)
        ]

    def remote_loads(heavy, piece):
        pairs = load_pairs(heavy, piece, 1 - core)
        return [
            to_partner(a, b, load_send.at[slot(piece) + i], load_recv.at[slot(piece) + i])
            for i, (a, b) in enumerate(pairs)
        ]

    def start_loads(heavy):
        pieces = [("meta", 0), ("kv", 0)] + [("q", kv) for kv in range(4)]
        pieces.insert(5, ("kv", 1))
        for piece in pieces:
            for copy in remote_loads(heavy, piece) + local_loads(heavy, piece):
                copy.start()

    def wait_loads(piece):
        def run(heavy):
            for copy in local_loads(heavy, piece):
                copy.wait()
            for copy in remote_loads(not heavy, piece):
                copy.wait_recv()

        by_role(run)

    def wait_sends():
        def run(heavy):
            for piece in [("meta", 0)] + [("q", kv) for kv in range(4)] + [("kv", 0), ("kv", 1)]:
                for copy in remote_loads(heavy, piece):
                    copy.wait_send()

        by_role(run)

    fetch = pltpu.make_async_copy(w_hbm, w_raw, w_sems.at[3, 0])
    fetch.start()
    barrier = pltpu.get_barrier_semaphore()
    for dim in "xyz":
        for by in (1, -1):
            pl.semaphore_signal(
                barrier, inc=1, device_id=rings[0].device(dim, by), device_id_type=MESH
            )
    pl.semaphore_signal(barrier, inc=1, device_id=partner, device_id_type=MESH)
    fetch.wait()
    shard = w_raw[...].astype(F32)
    w_split[:, :, :, 384:] = jnp.zeros((2, 3, 32, PART - 384), BF16)
    for side in range(2):
        for part in range(3):
            first = (side * 3 + part) * PART_COLS
            w_split[side, part, :, :PART_COLS] = shard[:, first : first + PART_COLS].astype(BF16)
    pl.semaphore_wait(barrier, 7)

    rows = pl.ds(pl.multiple_of(core * 32, 32), 32)
    chunk_remote = []
    for part, ring in enumerate(rings):
        target = ring.block((0, 0, 0)).at[rows]
        chunk_remote.append(
            to_partner(w_split.at[1 - core, part], target, w_sems.at[1, part], w_sems.at[2, part])
        )
    for copy in chunk_remote:
        copy.start()
    for part, ring in enumerate(rings):
        ring.block((0, 0, 0))[rows, :] = w_split[core, part]
    by_role(start_loads)
    for part, remote in enumerate(chunk_remote):
        remote.wait_send()
        other = pl.ds(pl.multiple_of(32 - core * 32, 32), 32)
        landed = rings[part].block((0, 0, 0)).at[other]
        to_partner(landed, landed, w_sems.at[1, part], w_sems.at[2, part]).wait_recv()

    def start(name):
        for copy in message(rings, name, send_sems, recv_sems):
            copy.start()

    def finish(name):
        for copy in message(rings, name, send_sems, recv_sems):
            copy.wait()

    for name in ("own", "l0", "f0"):
        start(name)
    wait_loads(("meta", 0))
    build_bias(meta_b, bias_b, NODES, NODES)
    build_bias(meta_l, bias_l, LIGHT, LIGHT)
    count_b, count_l = meta_b[16:17, :TILE], meta_l[16:17, :TILE]
    refs = (q_b, q_l, keys_b, values_b, keys_l, values_l, bias_b, bias_l, sinks, att, scores)

    def wide(meta):
        return jnp.concatenate([meta[17:18, :], meta[17:18, :]], axis=1)

    def att_half(side, step):
        return att.at[:, pl.ds(pl.multiple_of(side * HALF + step * 256, 256), 256)]

    def att_swap(step):
        own = att_half(core, step)
        return to_partner(own, own, att_send.at[step], att_recv.at[step])

    def per_step(step, carry):
        kv = lax.div(step, 2)
        for when, waits, starts in PLAN:

            @pl.when(step == when)
            def _():
                for name in waits:
                    finish(name)
                for name in starts:
                    start(name)

        @pl.when(lax.rem(step, 2) == 0)
        def _():
            pair = lax.div(kv, 2)
            second = lax.rem(kv, 2) == 1
            wait_loads(("q", kv))
            pl.when(jnp.logical_not(second))(lambda: wait_loads(("kv", pair)))
            lanes = pl.ds(pl.multiple_of(pair * 128, 128), 128)
            prepare(
                kc_b[:, lanes], vc_b[:, lanes], kt_b[:, lanes], vt_b[:, lanes], wide(meta_b),
                second, keys_b, values_b, NODES,
            )
            prepare(
                kc_l[:, lanes], vc_l[:, lanes], kt_l[:, lanes], vt_l[:, lanes], wide(meta_l),
                second, keys_l, values_l, LIGHT,
            )

        @pl.when(step == 0)
        def _():
            finish("own")
            for name in ("far", "l-", "l+", "f-", "f+"):
                start(name)

        attend_pairs(step, core, refs, (count_b, count_l))
        pl.when(step > 0)(lambda: att_swap(step - 1).start())
        return carry

    lax.fori_loop(0, 8, per_step, 0)
    wait_sends()
    att_swap(7).start()
    for step in range(8):
        att_swap(step).wait_send()
        other = att_half(1 - core, step)
        to_partner(other, other, att_send.at[step], att_recv.at[step]).wait_recv()

    def att_store(heavy):
        first, count = (0, NODES) if heavy else (NODES, LIGHT)
        return pltpu.make_async_copy(
            att.at[pl.ds(first, count)], att_hbm.at[pl.ds(0, count)], att_sem
        )

    by_role(lambda heavy: att_store(heavy).start())

    def proj_block(heavy, part):
        first, count = (0, NODES) if heavy else (NODES, LIGHT)
        return proj.at[part, pl.ds(0, PART_COLS), pl.ds(first, count)]

    def proj_place(heavy, side, part):
        count = NODES if heavy else LIGHT
        rows = pl.ds(pl.multiple_of((side * 3 + part) * PART_COLS, 32), PART_COLS)
        return proj_hbm.at[rows, pl.ds(0, count)]

    def proj_copies(heavy, part):
        own = pltpu.make_async_copy(
            proj_block(heavy, part), proj_place(heavy, core, part), proj_sem.at[part]
        )
        sent = to_partner(
            proj_block(not heavy, part), proj_place(not heavy, core, part), proj_send.at[part],
            proj_recv.at[part],
        )
        return own, sent

    def start_proj(heavy, part):
        own, sent = proj_copies(heavy, part)
        sent.start()
        own.start()

    def finish_proj(heavy, part):
        own, sent = proj_copies(heavy, part)
        own.wait()
        sent.wait_send()
        landed = proj_place(heavy, 1 - core, part)
        to_partner(landed, landed, proj_send.at[part], proj_recv.at[part]).wait_recv()

    def lanes_of(rows, first, count):
        return att[rows, pl.ds(pl.multiple_of(first, 128), count)]

    def terms(part, rows, last):
        ring = rings[part]
        pairs = []
        if part == 0:
            z_hi = lax.div(place["z"], 2)
            z_hi = 1 - z_hi if last else z_hi
            for y in range(4):
                pairs.append(
                    (lanes_of(rows, (2 * y + z_hi) * 512, 512), weights_0[y, z_hi].reshape(512, PART))
                )
        else:
            for by in (2,) if last else (0, 1, -1):
                at = ring.moved(ring.order[2], by)
                if part == 1:
                    left = [lanes_of(rows, g * 512 + at * 128, 128) for g in range(8)]
                    right = weights_1[:, :, at].reshape(1024, PART)
                    pairs.append((jnp.concatenate(left, axis=1), right))
                else:
                    pairs.append((lanes_of(rows, at * 1024, 1024), weights_2[at].reshape(1024, PART)))
        total = None
        for left, right in pairs:
            term = jnp.dot(left, right, preferred_element_type=F32)
            total = term if total is None else total + term
        return total

    row_blocks = (pl.ds(0, 384), pl.ds(384, 256))
    for part in range(3):
        for rows in row_blocks:
            partial[part, rows, :] = terms(part, rows, False)
    for name in ("back0", "back-", "back+", "back2"):
        finish(name)
    for part in range(3):
        for rows in row_blocks:
            total = partial[part, rows, :] + terms(part, rows, True)
            proj[part, :, rows] = total.T.astype(BF16)
        if part > 0:
            by_role(functools.partial(start_proj, part=part - 1))
    by_role(lambda heavy: att_store(heavy).wait())
    by_role(functools.partial(start_proj, part=2))
    for part in range(3):
        by_role(functools.partial(finish_proj, part=part))


def whole(sinks, *arrays):
    smem = pl.BlockSpec(memory_space=pltpu.SMEM)
    hbm = pl.BlockSpec(memory_space=pl.ANY)
    dma = pltpu.SemaphoreType.DMA

    def role(rows):
        return [
            pltpu.VMEM((rows, HALF), BF16),
            pltpu.VMEM((CACHE, 256), BF16),
            pltpu.VMEM((CACHE, 256), BF16),
            pltpu.VMEM((rows, 256), BF16),
            pltpu.VMEM((rows, 256), BF16),
            pltpu.VMEM((24, NODES), jnp.int32),
        ]

    return pl.pallas_call(
        whole_kernel,
        out_shape=(
            jax.ShapeDtypeStruct((NODES, 2 * HALF), BF16),
            jax.ShapeDtypeStruct((D, NODES), BF16),
        ),
        in_specs=[smem] + [hbm] * len(arrays),
        out_specs=(hbm, hbm),
        scratch_shapes=role(NODES)
        + role(LIGHT)
        + [pltpu.VMEM((4, 2, 4, 2, 64, PART), BF16)] * 3
        + [
            pltpu.VMEM((NODES + LIGHT, 2 * HALF), BF16),
            pltpu.VMEM((3, PART, NODES + LIGHT), BF16),
            pltpu.VMEM((3, NODES + LIGHT, PART), F32),
            pltpu.VMEM((32, D), BF16),
            pltpu.VMEM((2, 3, 32, PART), BF16),
            pltpu.VMEM((3, CACHE + NODES, TILE), F32),
            pltpu.VMEM((CACHE + NODES, 128), BF16),
            pltpu.VMEM((HD + SUMS, CACHE + NODES), BF16),
            pltpu.VMEM((CACHE + LIGHT, 128), BF16),
            pltpu.VMEM((HD + SUMS, CACHE + LIGHT), BF16),
            pltpu.VMEM((NODES, NODES), F32),
            pltpu.VMEM((LIGHT, LIGHT), F32),
            dma((len(NAMES), 3, 2)), dma((len(NAMES), 3, 2)),
            dma((14,)), dma((14,)), dma((14,)), dma((4, 3)),
            dma((8,)), dma((8,)), dma, dma((3,)), dma((3,)), dma((3,)),
        ],
        compiler_params=pltpu.CompilerParams(
            vmem_limit_bytes=60 * 1024 * 1024, collective_id=0, has_side_effects=True
        ),
        cost_estimate=pl.CostEstimate(
            flops=32 * (512 * 1536 + 128 * 1152) * 256, bytes_accessed=8 * 2**20, transcendentals=0
        ),
        name="whole",
    )(sinks, *arrays)


def keep_kernel(limit, att_in, proj_in, att_out, proj_out, att, proj, in_sems, out_sems):
    att_rows, proj_rows = NODES // KEEP, D // KEEP
    moves = []
    for i in range(KEEP):
        rows = pl.ds(i * att_rows, att_rows)
        moves.append((att_in.at[rows], att.at[rows], att_out.at[rows], rows))
        rows = pl.ds(i * proj_rows, proj_rows)
        moves.append((proj_in.at[rows], proj.at[rows], proj_out.at[rows], rows))
    reads = [pltpu.make_async_copy(m[0], m[1], in_sems.at[i]) for i, m in enumerate(moves)]
    writes = [pltpu.make_async_copy(m[1], m[2], out_sems.at[i]) for i, m in enumerate(moves)]
    for copy in reads:
        copy.start()
    for i, move in enumerate(moves):
        reads[i].wait()

        @pl.when(limit[0] < NODES)
        def _():
            if i % 2 == 0:
                if i // 2 * att_rows >= LIGHT:
                    att[move[3], :] = jnp.zeros((att_rows, 2 * HALF), BF16)
            else:
                proj[move[3], LIGHT:] = jnp.zeros((proj_rows, NODES - LIGHT), BF16)

        writes[i].start()
    for copy in writes:
        copy.wait()


def keep_live(limit, attended, projected):
    hbm = pl.BlockSpec(memory_space=pl.ANY)
    dma = pltpu.SemaphoreType.DMA
    return pl.pallas_call(
        keep_kernel,
        out_shape=(
            jax.ShapeDtypeStruct(attended.shape, BF16), jax.ShapeDtypeStruct(projected.shape, BF16)
        ),
        in_specs=[pl.BlockSpec(memory_space=pltpu.SMEM), hbm, hbm],
        out_specs=(hbm, hbm),
        scratch_shapes=[
            pltpu.VMEM(attended.shape, BF16), pltpu.VMEM(projected.shape, BF16),
            dma((2 * KEEP,)), dma((2 * KEEP,)),
        ],
        compiler_params=pltpu.CompilerParams(vmem_limit_bytes=60 * 1024 * 1024),
        name="keep",
    )(limit, attended, projected)


def on_device(
    q_nodes, k_cache, v_cache, k_tree, v_tree, anc_bits, node_count, cache_len, sinks, o_weight
):
    busy = lax.rem(lax.axis_index("gx") + lax.axis_index("core"), 2) == 0
    row = lax.broadcasted_iota(jnp.int32, (8, NODES), 0)
    counts = jnp.where(row == 0, node_count[0], cache_len[0])
    attended, projected = whole(
        sinks, q_nodes[0], k_cache[0], v_cache[0], k_tree[0], v_tree[0], anc_bits[0].T, counts, o_weight
    )
    limit = jnp.where(busy, NODES, LIGHT).astype(jnp.int32)[None]
    attended, projected = keep_live(limit, attended, projected)
    return attended[None], projected.T[None]


def solution(mesh):
    split = Mesh(mesh.devices.reshape(8, 8, 2), ("gx", "gyc", "core"))
    every = ("gx", "gyc", "core")
    placed = tuple([P(every)] * 8) + (P(), P(every))
    return jax.shard_map(
        on_device, mesh=split, in_specs=placed, out_specs=(P(every), P(every)), check_vma=False
    )
```

```python
import functools

import jax
import jax.numpy as jnp
from jax import lax
from jax.experimental import pallas as pl
from jax.experimental.pallas import tpu as pltpu
from jax.sharding import Mesh, PartitionSpec as P

HD = 64
NODES = 512
LIGHT = 128
KEEP = 4
CACHE = 1024
HALF = 2048
D = 2880
TILE = 256
SUMS = 16
EXP_SCALE = 0.125 * 1.4426950408889634
MASKED = -1.0e30
PART = 512
PART_COLS = 480
MESH = pl.DeviceIdType.MESH
WHERE = {"x": (2,), "y": (0,), "z": (1, 3)}
SIZES = (4, 2, 4, 2)
PLAN = (
    (1, ("far",), ("l2", "f2")),
    (2, ("l0", "l-", "l+", "l2"), ("line2", "face-", "face+")),
    (3, ("line2", "f0", "f-", "f+", "f2"), ("face2", "back0")),
    (6, ("face-", "face+"), ("back-", "back+")),
)
NAMES = (
    "own", "far", "l0", "l-", "l+", "l2", "line2", "f0", "f-", "f+", "f2", "face-", "face+",
    "face2", "back0", "back-", "back+", "back2",
)
LINES = {"0": 0, "-": -1, "+": 1, "2": 2}
F32 = jnp.float32
BF16 = jnp.bfloat16


def lane_ids(shape):
    return lax.broadcasted_iota(jnp.int32, shape, len(shape) - 1)


def row_ids(shape):
    return lax.broadcasted_iota(jnp.int32, shape, len(shape) - 2)


def build_bias(bits_ref, bias_ref, keys, nodes):
    shift = row_ids((32, nodes))
    for word in range(keys // 32):
        row = jnp.broadcast_to(bits_ref[word : word + 1, :nodes], (32, nodes))
        bit = jnp.bitwise_and(lax.shift_right_logical(row, shift), 1)
        bias_ref[word * 32 : word * 32 + 32, :] = jnp.where(bit > 0, 0.0, MASKED)


def spread_keys(pair, second):
    wide = pair.astype(F32)
    turned = pltpu.roll(wide, HD, 1)
    take_own = (lane_ids(wide.shape) < HD) == jnp.logical_not(second)
    return jnp.where(take_own, wide, turned)


def turn_values(pair, second):
    turned = pair.astype(F32).T
    return jnp.where(second, turned[HD:], turned[:HD])


def prepare(k_cache, v_cache, k_tree, v_tree, length, second, keys_ref, values_ref, tree):
    keys = spread_keys(k_cache, second)
    keys_ref[pl.ds(0, CACHE), :] = jnp.where(row_ids(keys.shape) < length[:, :128], keys, 0.0).astype(BF16)
    keys_ref[pl.ds(CACHE, tree), :] = spread_keys(k_tree, second).astype(BF16)
    values = turn_values(v_cache, second)
    live = lane_ids(values.shape) < length
    values_ref[pl.ds(0, HD), pl.ds(0, CACHE)] = jnp.where(live, values, 0.0).astype(BF16)
    live = lane_ids((SUMS, CACHE)) < length
    values_ref[pl.ds(HD, SUMS), pl.ds(0, CACHE)] = jnp.where(live, 1.0, 0.0).astype(BF16)
    values_ref[pl.ds(0, HD), pl.ds(CACHE, tree)] = turn_values(v_tree, second).astype(BF16)
    values_ref[pl.ds(HD, SUMS), pl.ds(CACHE, tree)] = jnp.ones((SUMS, tree), BF16)


def contract_last(a, b):
    return lax.dot_general(a, b, (((1,), (1,)), ((), ())), preferred_element_type=F32)


def fold_max(scores):
    rows = scores.shape[0]
    return jnp.max(scores.reshape(rows // 8, 8, TILE), axis=0)


class Unit:
    def __init__(self, keys, values, queries, bias, tree, sink, node_ok, scores):
        self.keys, self.values, self.queries, self.bias = keys, values, queries, bias
        self.sink, self.node_ok, self.scores = sink, node_ok, scores
        self.chunks = [(at, TILE) for at in range(0, CACHE, TILE)]
        self.chunks += [(CACHE + at, min(TILE, tree)) for at in range(0, tree, TILE)]
        self.peak = None
        self.total = None

    def score(self, number):
        at, count = self.chunks[number]
        scores = contract_last(self.keys[pl.ds(at, count), :], self.queries)
        if at >= CACHE:
            scores = scores + self.bias(at - CACHE, count)
        self.scores[pl.ds(at, count), :] = scores
        peak = fold_max(scores)
        self.peak = peak if self.peak is None else jnp.maximum(self.peak, peak)

    def settle(self):
        self.row_max = jnp.maximum(jnp.max(self.peak, axis=0, keepdims=True), self.sink)

    def weigh(self, number):
        at, count = self.chunks[number]
        weights = jnp.exp2((self.scores[pl.ds(at, count), :] - self.row_max) * EXP_SCALE)
        term = jnp.dot(
            self.values[:, pl.ds(at, count)], weights.astype(BF16), preferred_element_type=F32
        )
        self.total = term if self.total is None else self.total + term

    def result(self):
        denominator = self.total[HD : HD + 1] + jnp.exp2((self.sink - self.row_max) * EXP_SCALE)
        return self.total[:HD] * jnp.where(self.node_ok, 1.0 / denominator, 0.0)


def attend_pairs(step, core, refs, counts):
    (q_busy, q_light, keys_b, values_b, keys_l, values_l, bias_b, bias_l, sinks, att, scores) = refs
    count_b, count_l = counts
    columns = lane_ids((1, TILE))
    units, outputs = [], {}
    for inner in range(2):
        pair = 2 * step + inner
        lanes = pl.ds(pl.multiple_of(pair * 128, 128), 128)
        out_lanes = pl.ds(pl.multiple_of(core * HALF + pair * 128, 128), 128)
        sink_even = sinks[core * 32 + 2 * pair] * 8.0
        sink_odd = sinks[core * 32 + 2 * pair + 1] * 8.0
        for tile in range(NODES // TILE):
            rows = pl.ds(tile * TILE, TILE)
            for odd, sink in enumerate((sink_even, sink_odd)):
                both = q_busy[rows, lanes]
                own = (lane_ids(both.shape) < HD) == (odd == 0)
                units.append(
                    Unit(
                        keys_b, values_b, jnp.where(own, both, jnp.zeros_like(both)),
                        lambda at, count, rows=rows: bias_b[pl.ds(at, count), rows],
                        (tile + 1) * TILE, sink, columns + tile * TILE < count_b,
                        scores.at[len(units) % 3],
                    )
                )
            outputs[len(units) - 1] = (rows, out_lanes)
        both = q_light[:, lanes]
        left = lane_ids(both.shape) < HD
        zero = jnp.zeros_like(both)
        both = jnp.concatenate([jnp.where(left, both, zero), jnp.where(left, zero, both)], axis=0)
        units.append(
            Unit(
                keys_l, values_l, both,
                lambda at, count: jnp.concatenate([bias_l[...], bias_l[...]], axis=1), LIGHT,
                jnp.where(columns < LIGHT, sink_even, sink_odd),
                jnp.where(columns < LIGHT, columns, columns - LIGHT) < count_l,
                scores.at[len(units) % 3],
            )
        )
        outputs[len(units) - 1] = (None, out_lanes)
    results = []
    for number in range(len(units) + 2):
        ahead = units[number] if number < len(units) else None
        behind = units[number - 2] if number >= 2 else None
        for chunk in range(6):
            if ahead is not None and chunk < len(ahead.chunks):
                ahead.score(chunk)
            if behind is not None and chunk < len(behind.chunks):
                behind.weigh(chunk)
        if behind is not None:
            results.append(behind.result())
        if ahead is not None:
            ahead.settle()
        if number - 2 in outputs:
            rows, out_lanes = outputs[number - 2]
            if rows is None:
                rows = pl.ds(NODES, LIGHT)
                pieces = [results[-1][:, :LIGHT], results[-1][:, LIGHT:]]
            else:
                pieces = results[-2:]
            att[rows, out_lanes] = jnp.concatenate(pieces, axis=0).T.astype(BF16)


class Ring:
    def __init__(self, order, place, core, weights):
        self.order, self.place, self.core, self.weights = order, place, core, weights

    def moved(self, dim, by):
        return lax.rem(self.place[dim] + 4 + by, 4)

    def device(self, dim, by):
        at = dict(self.place)
        at[dim] = self.moved(dim, by)
        x, y, z = at["x"], at["y"], at["z"]
        return (y * 2 + lax.div(z, 2), x * 2 + lax.rem(z, 2), self.core)

    def block(self, offsets, whole=False, half=None):
        at = {dim: self.moved(dim, by) for dim, by in zip(self.order, offsets)}
        index = [at["y"], lax.div(at["z"], 2), at["x"], lax.rem(at["z"], 2), slice(None)]
        axes = WHERE[self.order[0]] if whole else (4,)
        if whole:
            for axis in axes:
                index[axis] = slice(None)
        if half is not None:
            size = (SIZES[axes[0]] if whole else 64) // 2
            index[axes[0]] = pl.ds(half * size, size)
        return self.weights.at[tuple(index)]

    def send(self, name, side):
        by = (1, -1)[side]
        if name == "own":
            return 0, self.block((0, 0, 0))
        if name == "far":
            return 0, self.block((-by, 0, 0), half=side)
        if name == "line2":
            return 1, self.block((0, -by, 0), whole=True, half=side)
        line = LINES[name[-1]]
        if len(name) == 2:
            return {"l": 1, "f": 2}[name[0]], self.block((line, 0, 0))
        if name.startswith("face"):
            return 2, self.block((0, line, 0), whole=True)
        return 2, self.block((0, line, -by), whole=True, half=side)


def message(rings, name, send_sems, recv_sems):
    number = NAMES.index(name)
    copies = []
    for part, ring in enumerate(rings):
        for side in range(2):
            axis, block = ring.send(name, side)
            copies.append(
                pltpu.make_async_remote_copy(
                    src_ref=block, dst_ref=block,
                    send_sem=send_sems.at[number, part, side],
                    recv_sem=recv_sems.at[number, part, side],
                    device_id=ring.device(ring.order[axis], (1, -1)[side]),
                    device_id_type=MESH,
                )
            )
    return copies


def whole_kernel(
    sinks, q_hbm, kc_hbm, vc_hbm, kt_hbm, vt_hbm, bits_hbm, count_hbm, w_hbm, att_hbm, proj_hbm,
    q_b, kc_b, vc_b, kt_b, vt_b, meta_b, q_l, kc_l, vc_l, kt_l, vt_l, meta_l,
    weights_0, weights_1, weights_2, att, proj, partial, w_raw, w_split, scores, keys_b, values_b, keys_l, values_l, bias_b, bias_l,
    send_sems, recv_sems, load_sems, load_send, load_recv, w_sems, att_send, att_recv, att_sem,
    proj_send, proj_recv, proj_sem,
):
    gx, gyc, core = lax.axis_index("gx"), lax.axis_index("gyc"), lax.axis_index("core")
    partner = (gx, gyc, 1 - core)
    busy = lax.rem(gx + core, 2) == 0
    place = {
        "x": lax.div(gyc, 2), "y": lax.div(gx, 2), "z": lax.rem(gx, 2) * 2 + lax.rem(gyc, 2)
    }
    weights = (weights_0, weights_1, weights_2)
    rings = [Ring(order, place, core, w) for order, w in zip(("xyz", "yzx", "zxy"), weights)]

    def by_role(run):
        pl.when(busy)(lambda: run(True))
        pl.when(jnp.logical_not(busy))(lambda: run(False))

    def to_partner(source, target, send, recv):
        return pltpu.make_async_remote_copy(
            src_ref=source, dst_ref=target, send_sem=send, recv_sem=recv, device_id=partner,
            device_id_type=MESH,
        )

    def load_pairs(heavy, piece, half):
        rows, q, kc, vc, kt, vt, meta = (
            (NODES, q_b, kc_b, vc_b, kt_b, vt_b, meta_b)
            if heavy
            else (LIGHT, q_l, kc_l, vc_l, kt_l, vt_l, meta_l)
        )
        if piece[0] == "q":
            return [
                (
                    q_hbm.at[pl.ds(0, rows), pl.ds(half * HALF + piece[1] * 512, 512)],
                    q.at[:, pl.ds(pl.multiple_of(piece[1] * 512, 512), 512)],
                )
            ]
        if piece[0] == "meta":
            return [(bits_hbm, meta.at[pl.ds(0, 16)]), (count_hbm, meta.at[pl.ds(16, 8)])]
        source = pl.ds(half * 256 + piece[1] * 128, 128)
        target = pl.ds(pl.multiple_of(piece[1] * 128, 128), 128)
        return [
            (kc_hbm.at[:, source], kc.at[:, target]),
            (vc_hbm.at[:, source], vc.at[:, target]),
            (kt_hbm.at[pl.ds(0, rows), source], kt.at[:, target]),
            (vt_hbm.at[pl.ds(0, rows), source], vt.at[:, target]),
        ]

    def slot(piece):
        return {"meta": 0, "q": 2, "kv": 6}[piece[0]] + piece[1] * (4 if piece[0] == "kv" else 1)

    def local_loads(heavy, piece):
        pairs = load_pairs(heavy, piece, core)
        return [
            pltpu.make_async_copy(a, b, load_sems.at[slot(piece) + i])
            for i, (a, b) in enumerate(pairs)
        ]

    def remote_loads(heavy, piece):
        pairs = load_pairs(heavy, piece, 1 - core)
        return [
            to_partner(a, b, load_send.at[slot(piece) + i], load_recv.at[slot(piece) + i])
            for i, (a, b) in enumerate(pairs)
        ]

    def start_loads(heavy):
        pieces = [("meta", 0), ("kv", 0)] + [("q", kv) for kv in range(4)]
        pieces.insert(5, ("kv", 1))
        for piece in pieces:
            for copy in remote_loads(heavy, piece) + local_loads(heavy, piece):
                copy.start()

    def wait_loads(piece):
        def run(heavy):
            for copy in local_loads(heavy, piece):
                copy.wait()
            for copy in remote_loads(not heavy, piece):
                copy.wait_recv()

        by_role(run)

    def wait_sends():
        def run(heavy):
            for piece in [("meta", 0)] + [("q", kv) for kv in range(4)] + [("kv", 0), ("kv", 1)]:
                for copy in remote_loads(heavy, piece):
                    copy.wait_send()

        by_role(run)

    fetch = pltpu.make_async_copy(w_hbm, w_raw, w_sems.at[3, 0])
    fetch.start()
    barrier = pltpu.get_barrier_semaphore()
    for dim in "xyz":
        for by in (1, -1):
            pl.semaphore_signal(
                barrier, inc=1, device_id=rings[0].device(dim, by), device_id_type=MESH
            )
    pl.semaphore_signal(barrier, inc=1, device_id=partner, device_id_type=MESH)
    fetch.wait()
    shard = w_raw[...].astype(F32)
    w_split[:, :, :, 384:] = jnp.zeros((2, 3, 32, PART - 384), BF16)
    for side in range(2):
        for part in range(3):
            first = (side * 3 + part) * PART_COLS
            w_split[side, part, :, :PART_COLS] = shard[:, first : first + PART_COLS].astype(BF16)
    pl.semaphore_wait(barrier, 7)

    rows = pl.ds(pl.multiple_of(core * 32, 32), 32)
    chunk_remote = []
    for part, ring in enumerate(rings):
        target = ring.block((0, 0, 0)).at[rows]
        chunk_remote.append(
            to_partner(w_split.at[1 - core, part], target, w_sems.at[1, part], w_sems.at[2, part])
        )
    for copy in chunk_remote:
        copy.start()
    for part, ring in enumerate(rings):
        ring.block((0, 0, 0))[rows, :] = w_split[core, part]
    by_role(start_loads)
    for part, remote in enumerate(chunk_remote):
        remote.wait_send()
        other = pl.ds(pl.multiple_of(32 - core * 32, 32), 32)
        landed = rings[part].block((0, 0, 0)).at[other]
        to_partner(landed, landed, w_sems.at[1, part], w_sems.at[2, part]).wait_recv()

    def start(name):
        for copy in message(rings, name, send_sems, recv_sems):
            copy.start()

    def finish(name):
        for copy in message(rings, name, send_sems, recv_sems):
            copy.wait()

    for name in ("own", "l0", "f0"):
        start(name)
    wait_loads(("meta", 0))
    build_bias(meta_b, bias_b, NODES, NODES)
    build_bias(meta_l, bias_l, LIGHT, LIGHT)
    count_b, count_l = meta_b[16:17, :TILE], meta_l[16:17, :TILE]
    refs = (q_b, q_l, keys_b, values_b, keys_l, values_l, bias_b, bias_l, sinks, att, scores)

    def wide(meta):
        return jnp.concatenate([meta[17:18, :], meta[17:18, :]], axis=1)

    def att_half(side, step):
        return att.at[:, pl.ds(pl.multiple_of(side * HALF + step * 256, 256), 256)]

    def att_swap(step):
        own = att_half(core, step)
        return to_partner(own, own, att_send.at[step], att_recv.at[step])

    def per_step(step, carry):
        kv = lax.div(step, 2)
        for when, waits, starts in PLAN:

            @pl.when(step == when)
            def _():
                for name in waits:
                    finish(name)
                for name in starts:
                    start(name)

        @pl.when(lax.rem(step, 2) == 0)
        def _():
            pair = lax.div(kv, 2)
            second = lax.rem(kv, 2) == 1
            wait_loads(("q", kv))
            pl.when(jnp.logical_not(second))(lambda: wait_loads(("kv", pair)))
            lanes = pl.ds(pl.multiple_of(pair * 128, 128), 128)
            prepare(
                kc_b[:, lanes], vc_b[:, lanes], kt_b[:, lanes], vt_b[:, lanes], wide(meta_b),
                second, keys_b, values_b, NODES,
            )
            prepare(
                kc_l[:, lanes], vc_l[:, lanes], kt_l[:, lanes], vt_l[:, lanes], wide(meta_l),
                second, keys_l, values_l, LIGHT,
            )

        @pl.when(step == 0)
        def _():
            finish("own")
            for name in ("far", "l-", "l+", "f-", "f+"):
                start(name)

        attend_pairs(step, core, refs, (count_b, count_l))
        pl.when(step > 0)(lambda: att_swap(step - 1).start())
        return carry

    lax.fori_loop(0, 8, per_step, 0)
    wait_sends()
    att_swap(7).start()
    finish("face2")
    start("back2")
    for step in range(8):
        att_swap(step).wait_send()
        other = att_half(1 - core, step)
        to_partner(other, other, att_send.at[step], att_recv.at[step]).wait_recv()

    def att_store(heavy):
        first, count = (0, NODES) if heavy else (NODES, LIGHT)
        return pltpu.make_async_copy(
            att.at[pl.ds(first, count)], att_hbm.at[pl.ds(0, count)], att_sem
        )

    by_role(lambda heavy: att_store(heavy).start())

    def proj_block(heavy, part):
        first, count = (0, NODES) if heavy else (NODES, LIGHT)
        return proj.at[part, pl.ds(0, PART_COLS), pl.ds(first, count)]

    def proj_place(heavy, side, part):
        count = NODES if heavy else LIGHT
        rows = pl.ds(pl.multiple_of((side * 3 + part) * PART_COLS, 32), PART_COLS)
        return proj_hbm.at[rows, pl.ds(0, count)]

    def proj_copies(heavy, part):
        own = pltpu.make_async_copy(
            proj_block(heavy, part), proj_place(heavy, core, part), proj_sem.at[part]
        )
        sent = to_partner(
            proj_block(not heavy, part), proj_place(not heavy, core, part), proj_send.at[part],
            proj_recv.at[part],
        )
        return own, sent

    def start_proj(heavy, part):
        own, sent = proj_copies(heavy, part)
        sent.start()
        own.start()

    def finish_proj(heavy, part):
        own, sent = proj_copies(heavy, part)
        own.wait()
        sent.wait_send()
        landed = proj_place(heavy, 1 - core, part)
        to_partner(landed, landed, proj_send.at[part], proj_recv.at[part]).wait_recv()

    def lanes_of(rows, first, count):
        return att[rows, pl.ds(pl.multiple_of(first, 128), count)]

    def terms(part, rows, last):
        ring = rings[part]
        pairs = []
        if part == 0:
            z_hi = lax.div(place["z"], 2)
            z_hi = 1 - z_hi if last else z_hi
            for y in range(4):
                pairs.append(
                    (lanes_of(rows, (2 * y + z_hi) * 512, 512), weights_0[y, z_hi].reshape(512, PART))
                )
        else:
            for by in (2,) if last else (0, 1, -1):
                at = ring.moved(ring.order[2], by)
                if part == 1:
                    left = [lanes_of(rows, g * 512 + at * 128, 128) for g in range(8)]
                    right = weights_1[:, :, at].reshape(1024, PART)
                    pairs.append((jnp.concatenate(left, axis=1), right))
                else:
                    pairs.append((lanes_of(rows, at * 1024, 1024), weights_2[at].reshape(1024, PART)))
        total = None
        for left, right in pairs:
            term = jnp.dot(left, right, preferred_element_type=F32)
            total = term if total is None else total + term
        return total

    row_blocks = (pl.ds(0, 384), pl.ds(384, 256))
    for part in range(3):
        for rows in row_blocks:
            partial[part, rows, :] = terms(part, rows, False)
    for name in ("back0", "back-", "back+", "back2"):
        finish(name)
    for part in range(3):
        for rows in row_blocks:
            total = partial[part, rows, :] + terms(part, rows, True)
            proj[part, :, rows] = total.T.astype(BF16)
        if part > 0:
            by_role(functools.partial(start_proj, part=part - 1))
    by_role(lambda heavy: att_store(heavy).wait())
    by_role(functools.partial(start_proj, part=2))
    for part in range(3):
        by_role(functools.partial(finish_proj, part=part))


def whole(sinks, *arrays):
    smem = pl.BlockSpec(memory_space=pltpu.SMEM)
    hbm = pl.BlockSpec(memory_space=pl.ANY)
    dma = pltpu.SemaphoreType.DMA

    def role(rows):
        return [
            pltpu.VMEM((rows, HALF), BF16),
            pltpu.VMEM((CACHE, 256), BF16),
            pltpu.VMEM((CACHE, 256), BF16),
            pltpu.VMEM((rows, 256), BF16),
            pltpu.VMEM((rows, 256), BF16),
            pltpu.VMEM((24, NODES), jnp.int32),
        ]

    return pl.pallas_call(
        whole_kernel,
        out_shape=(
            jax.ShapeDtypeStruct((NODES, 2 * HALF), BF16),
            jax.ShapeDtypeStruct((D, NODES), BF16),
        ),
        in_specs=[smem] + [hbm] * len(arrays),
        out_specs=(hbm, hbm),
        scratch_shapes=role(NODES)
        + role(LIGHT)
        + [pltpu.VMEM((4, 2, 4, 2, 64, PART), BF16)] * 3
        + [
            pltpu.VMEM((NODES + LIGHT, 2 * HALF), BF16),
            pltpu.VMEM((3, PART, NODES + LIGHT), BF16),
            pltpu.VMEM((3, NODES + LIGHT, PART), F32),
            pltpu.VMEM((32, D), BF16),
            pltpu.VMEM((2, 3, 32, PART), BF16),
            pltpu.VMEM((3, CACHE + NODES, TILE), F32),
            pltpu.VMEM((CACHE + NODES, 128), BF16),
            pltpu.VMEM((HD + SUMS, CACHE + NODES), BF16),
            pltpu.VMEM((CACHE + LIGHT, 128), BF16),
            pltpu.VMEM((HD + SUMS, CACHE + LIGHT), BF16),
            pltpu.VMEM((NODES, NODES), F32),
            pltpu.VMEM((LIGHT, LIGHT), F32),
            dma((len(NAMES), 3, 2)), dma((len(NAMES), 3, 2)),
            dma((14,)), dma((14,)), dma((14,)), dma((4, 3)),
            dma((8,)), dma((8,)), dma, dma((3,)), dma((3,)), dma((3,)),
        ],
        compiler_params=pltpu.CompilerParams(
            vmem_limit_bytes=60 * 1024 * 1024, collective_id=0, has_side_effects=True
        ),
        cost_estimate=pl.CostEstimate(
            flops=32 * (512 * 1536 + 128 * 1152) * 256, bytes_accessed=8 * 2**20, transcendentals=0
        ),
        name="whole",
    )(sinks, *arrays)


def keep_kernel(limit, att_in, proj_in, att_out, proj_out, att, proj, in_sems, out_sems):
    att_rows, proj_rows = NODES // KEEP, D // KEEP
    moves = []
    for i in range(KEEP):
        rows = pl.ds(i * att_rows, att_rows)
        moves.append((att_in.at[rows], att.at[rows], att_out.at[rows], rows))
        rows = pl.ds(i * proj_rows, proj_rows)
        moves.append((proj_in.at[rows], proj.at[rows], proj_out.at[rows], rows))
    reads = [pltpu.make_async_copy(m[0], m[1], in_sems.at[i]) for i, m in enumerate(moves)]
    writes = [pltpu.make_async_copy(m[1], m[2], out_sems.at[i]) for i, m in enumerate(moves)]
    for copy in reads:
        copy.start()
    for i, move in enumerate(moves):
        reads[i].wait()

        @pl.when(limit[0] < NODES)
        def _():
            if i % 2 == 0:
                if i // 2 * att_rows >= LIGHT:
                    att[move[3], :] = jnp.zeros((att_rows, 2 * HALF), BF16)
            else:
                proj[move[3], LIGHT:] = jnp.zeros((proj_rows, NODES - LIGHT), BF16)

        writes[i].start()
    for copy in writes:
        copy.wait()


def keep_live(limit, attended, projected):
    hbm = pl.BlockSpec(memory_space=pl.ANY)
    dma = pltpu.SemaphoreType.DMA
    return pl.pallas_call(
        keep_kernel,
        out_shape=(
            jax.ShapeDtypeStruct(attended.shape, BF16), jax.ShapeDtypeStruct(projected.shape, BF16)
        ),
        in_specs=[pl.BlockSpec(memory_space=pltpu.SMEM), hbm, hbm],
        out_specs=(hbm, hbm),
        scratch_shapes=[
            pltpu.VMEM(attended.shape, BF16), pltpu.VMEM(projected.shape, BF16),
            dma((2 * KEEP,)), dma((2 * KEEP,)),
        ],
        compiler_params=pltpu.CompilerParams(vmem_limit_bytes=60 * 1024 * 1024),
        name="keep",
    )(limit, attended, projected)


def on_device(
    q_nodes, k_cache, v_cache, k_tree, v_tree, anc_bits, node_count, cache_len, sinks, o_weight
):
    busy = lax.rem(lax.axis_index("gx") + lax.axis_index("core"), 2) == 0
    row = lax.broadcasted_iota(jnp.int32, (8, NODES), 0)
    counts = jnp.where(row == 0, node_count[0], cache_len[0])
    attended, projected = whole(
        sinks, q_nodes[0], k_cache[0], v_cache[0], k_tree[0], v_tree[0], anc_bits[0].T, counts, o_weight
    )
    limit = jnp.where(busy, NODES, LIGHT).astype(jnp.int32)[None]
    attended, projected = keep_live(limit, attended, projected)
    return attended[None], projected.T[None]


def solution(mesh):
    split = Mesh(mesh.devices.reshape(8, 8, 2), ("gx", "gyc", "core"))
    every = ("gx", "gyc", "core")
    placed = tuple([P(every)] * 8) + (P(), P(every))
    return jax.shard_map(
        on_device, mesh=split, in_specs=placed, out_specs=(P(every), P(every)), check_vma=False
    )
```
